256 devices in a mesh: freq: 16 (over y, x), param: 4 (over z_hi, core), sens: 4 (over z_lo).
Axes of the slice: x: 4, y: 4, z: 8 (z_hi: 2, z_lo: 4; z = z_hi * 4 + z_lo), core: 2. Of those that a mesh axis runs over, the one named last changes fastest.
Arguments:
- series: bfloat16 [8, 600, 416], P(None, 'sens', 'freq'), may hold values from -6 to 6
- kernel: bfloat16 [2, 256, 600, 4096], P(None, 'freq', 'sens', 'param'), may hold values from -0.1875 to 0.1875
- prior_spectrum: float32 [256], P('freq'), may hold values from 0.3 to 1.5
- prior_scale: float32 [4096], P('param'), may hold values from 0.5 to 2
Outputs:
- adjoint_map: float32 [416, 8, 4096], P('freq', 'sens', 'param')
The draws below stay inside these ranges and needn't reach their ends.
All inputs are finite; a program needn't handle non-finite values.
Results may differ from the reference program's by a relative error of at most 0.0047.
Values may be sent and summed in bfloat16 or wider, within the bound.
A program may use at most 64 MiB of HBM per device.

```python
import math
import jax
import jax.numpy as jnp
from jax import lax

SENSORS = 600
LEN = 840
NB = 256
NT = 416
NP = 4096
PROBES = 8


def level_of(rng, extent, pieces, smallest, high):
    def one(position, blocks):
        steps = jax.random.uniform(jax.random.fold_in(jax.random.fold_in(rng, 6), position), (blocks,), jnp.float32, smallest / len(pieces), high / len(pieces))
        return jnp.repeat(jnp.exp(steps), extent[position] // blocks).reshape((-1,) + (1,) * (len(extent) - position - 1))

    level = one(*pieces[0])
    for cut in pieces[1:]:
        level = level * one(*cut)
    return level


def noise(rng, extent, width, reach, cuts=(), kind=jnp.bfloat16):
    entries = jax.random.normal(rng, extent, jnp.float32) * width
    if len(cuts) > 0:
        entries = level_of(rng, extent, cuts, -0.22, 0.18) * entries
    return jnp.clip(entries, min=-reach, max=reach).astype(kind)


def setup_inputs(seed: int = 0) -> dict:
    key_of = jax.random.split(jax.random.key(seed), 5)
    series = noise(key_of[0], (PROBES, SENSORS, NT), 1.0, 6.0, ((1, 4), (2, 16)))
    kernel = noise(key_of[1], (2, NB, SENSORS, NP), (2 * SENSORS) ** -0.5, 0.1875, ((1, 16), (2, 4), (3, 4)))
    prior_spectrum = jnp.clip(jnp.exp(math.log(1.5) - 1.60943787 * jax.random.uniform(key_of[2], (NB,), jnp.float32) ** level_of(key_of[2], (NB,), ((0, 16),), -0.2, 0.2)), 0.3, 1.5)
    prior_scale = jnp.clip(jnp.exp(math.log(2.0) - 1.3862944 * jax.random.uniform(key_of[3], (NP,), jnp.float32) ** level_of(key_of[3], (NP,), ((0, 4),), -0.2, 0.2)), 0.5, 2.0)
    return {"series": series, "kernel": kernel, "prior_spectrum": prior_spectrum, "prior_scale": prior_scale}


def phase_tables(bin_count, time_count):
    bin_index = jnp.arange(bin_count, dtype=jnp.int32)
    time_index = jnp.arange(time_count, dtype=jnp.int32)
    product = time_index[:, None] * bin_index[None, :] % LEN
    phase_angle = product.astype(jnp.float32) * (2.0 * math.pi / LEN)
    return (jnp.cos(phase_angle), jnp.sin(phase_angle))

def reference(series, kernel, prior_spectrum, prior_scale):
    highest = lax.Precision.HIGHEST
    cosine, sine_part = phase_tables(NB, NT)
    flat_rows = series.astype(jnp.float32).reshape(PROBES * SENSORS, NT)
    norm_time = 1.0 / math.sqrt(NT)
    spec_re = (jnp.dot(flat_rows, cosine, precision=highest) * norm_time).astype(jnp.bfloat16)
    spec_im = (-jnp.dot(flat_rows, sine_part, precision=highest) * norm_time).astype(jnp.bfloat16)
    spec_re = spec_re.reshape(PROBES, SENSORS, NB).transpose(2, 1, 0)
    spec_im = spec_im.reshape(PROBES, SENSORS, NB).transpose(2, 1, 0)

    def one_bin(index):
        kern_re = kernel[0, index]
        kern_im = kernel[1, index]
        data_re = spec_re[index].T
        data_im = spec_im[index].T
        real_part = jnp.dot(data_re, kern_re, preferred_element_type=jnp.float32) + jnp.dot(data_im, kern_im, preferred_element_type=jnp.float32)
        imag_part = jnp.dot(data_im, kern_re, preferred_element_type=jnp.float32) - jnp.dot(data_re, kern_im, preferred_element_type=jnp.float32)
        return jnp.stack([real_part, imag_part])
    spectra = lax.map(one_bin, jnp.arange(NB, dtype=jnp.int32))
    weights = prior_spectrum / math.sqrt(NB)
    scaled_spec = spectra * weights[:, None, None, None]
    image_re = scaled_spec[:, 0].reshape(NB, PROBES * NP)
    image_im = scaled_spec[:, 1].reshape(NB, PROBES * NP)
    image_field = jnp.dot(cosine, image_re, precision=highest) - jnp.dot(sine_part, image_im, precision=highest)
    image_field = image_field.reshape(NT, PROBES, NP)
    weighted = image_field * prior_scale
    padded = jnp.pad(weighted, ((0, 0), (0, 0), (1, 1)))
    smooth = 0.5 * weighted + 0.25 * (padded[:, :, :-2] + padded[:, :, 2:])
    return smooth * prior_scale
```

```python
import functools
import math

import jax
import jax.numpy as jnp
from jax import lax
from jax.experimental import pallas as pl
from jax.experimental.pallas import tpu as pltpu
from jax.sharding import PartitionSpec as P

LEN = 840
MESH = pl.DeviceIdType.MESH
F32, BF16 = jnp.float32, jnp.bfloat16
CHUNKS = ((0, 7), (1, 2), (3, 4), (5, 6))
READY = ((), (0, 1), (2, 3), (4, 5, 6, 7))


def iota(shape, dim):
    return lax.broadcasted_iota(jnp.int32, shape, dim)


def turned_cos(bins, times, part):
    turn = bins.astype(F32) * times.astype(F32) + (LEN // 4) * part.astype(F32)
    turn = turn - LEN * jnp.floor(turn * (1.0 / LEN) + 0.5)
    half = turn * (math.pi / LEN)
    square = half * half
    term = 1.0 / 6227020800.0
    for coef in (-1.0 / 39916800.0, 1.0 / 362880.0, -1.0 / 5040.0, 1.0 / 120.0, -1.0 / 6.0, 1.0):
        term = term * square + coef
    sine = half * term
    return 1.0 - 2.0 * sine * sine


def split(x):
    high = x.astype(BF16)
    return high, (x - high.astype(F32)).astype(BF16)


def kernel(
    series_ref, kern_ref, prior_ref, scale_ref, out_ref,
    ser_v, kern_v, by_time, turned, arecv, bsend, brecv, packed, lhs_re, lhs_im, zsend, zrecv, zfull,
    hsend, hrecv, wsend, wrecv, isend, irecv, table_hi, table_lo,
    local_sem, send_sem, recv_sem, zsend_sem, zrecv_sem, hsend_sem, hrecv_sem,
):
    f, par, s = lax.axis_index("freq"), lax.axis_index("param"), lax.axis_index("sens")
    y, x = f // 4, f % 4
    core = par % 2
    sensors = ser_v.shape[2]
    row = kern_v.shape[4] // 128
    rest_of = sensors - 128
    first_at = lambda j: j * (1 + 3 * core) + 4 * y * (1 - core) + x * core
    second_at = lambda m: m * (4 - 3 * core) + x * (1 - core) + 4 * y * core
    first_pos = x * (1 - core) + y * core
    second_pos = y * (1 - core) + x * core

    series_in = pltpu.make_async_copy(series_ref, ser_v, local_sem.at[0])
    series_in.start()
    kernel_in = []
    for p in range(2):
        for h in range(2):
            kernel_in.append(
                pltpu.make_async_copy(
                    kern_ref.at[p, :, pl.ds(8 * h, 8)], kern_v.at[h, p], local_sem.at[1 + 2 * h + p]
                )
            )
            kernel_in[-1].start()

    barrier = pltpu.get_barrier_semaphore()
    for o in range(1, 16):
        pl.semaphore_signal(barrier, 1, device_id={"freq": (f + o) % 16}, device_id_type=MESH)
    for o in range(1, 4):
        pl.semaphore_signal(barrier, 1, device_id={"sens": (s + o) % 4}, device_id_type=MESH)
    other = par + 1 - 2 * core
    for m in range(4):
        source = m * (1 + 3 * core) + 4 * y * (1 - core) + x * core
        pl.semaphore_signal(barrier, 1, device_id={"freq": source, "param": other}, device_id_type=MESH)

    @pl.when(par == 1)
    def _():
        pl.semaphore_signal(barrier, 1, device_id={"param": 2}, device_id_type=MESH)

    @pl.when(par == 2)
    def _():
        pl.semaphore_signal(barrier, 1, device_id={"param": 1}, device_id_type=MESH)

    ri, ci = iota((128, 128), 0), iota((128, 128), 1)
    bins = 16 * second_at(ri >> 5) + (ri & 15)
    inside = ci & 31
    times = 26 * first_at(ci >> 5) + inside
    forward = jnp.where(inside < 26, turned_cos(bins, times, (ri >> 4) & 1), 0.0)
    fwd_hi, fwd_lo = split(forward)

    turned[:, 512:640] = jnp.zeros((32, 128), F32)
    turned[24:32, :] = jnp.zeros((8, 640), F32)
    series_in.wait()
    by_time[0] = ser_v[:, :, 0:128].astype(F32).reshape(208, 128)
    by_time[1, :, 0:rest_of] = ser_v[:, :, 128:sensors].astype(F32).reshape(208, rest_of)
    for i in range(4):
        rows = pl.ds(4 * core + i, 26, stride=8)
        turned[0:26, 128 * i : 128 * i + 128] = by_time[0, rows, :]
        turned[0:26, 512 + 32 * i : 512 + 32 * i + rest_of] = by_time[1, rows, :][:, 0:rest_of]
    arecv[first_pos] = turned[...].astype(BF16)

    pl.semaphore_wait(barrier, 22 + jnp.where((par == 1) | (par == 2), 1, 0))

    for o in range(1, 4):
        pltpu.make_async_remote_copy(
            arecv.at[first_pos], arecv.at[first_pos], send_sem.at[0], recv_sem.at[0],
            device_id={"freq": first_at((first_pos + o) % 4)}, device_id_type=MESH,
        ).start()

    @pl.loop(0, 16)
    def _(b):
        ti, ki = iota((32, 512), 0), iota((32, 512), 1)
        values = turned_cos(((ki >> 5) << 4) + ((ki >> 4) & 1) * 8 + (ki & 7), 26 * b + ti, (ki >> 3) & 1)
        high, low = split(values)
        rows = pl.ds(pl.multiple_of(32 * b, 32), 32)
        table_hi[rows, :] = high
        table_lo[rows, :] = low

    def drain(like, sem):
        pltpu.make_async_copy(like, like, sem).wait()

    drain(arecv.at[pl.ds(0, 3)], recv_sem.at[0])
    gathered = arecv[...].reshape(128, 640)
    spec = jnp.dot(fwd_hi, gathered, preferred_element_type=F32)
    spec = spec + jnp.dot(fwd_lo, gathered, preferred_element_type=F32)
    spec = spec * (1.0 / math.sqrt(416.0))
    bsend[...] = spec.astype(BF16).reshape(4, 32, 640)
    for o in range(4):
        m = (second_pos + o) % 4
        for c in range(2):
            if o + c > 0:
                target = par + (1 - 2 * core) * c
                pltpu.make_async_remote_copy(
                    bsend.at[m], brecv.at[4 * core + second_pos], send_sem.at[1], recv_sem.at[1],
                    device_id={"freq": second_at(m), "param": target}, device_id_type=MESH,
                ).start()
    brecv[4 * core + second_pos] = bsend[second_pos]
    drain(brecv.at[pl.ds(0, 7)], recv_sem.at[1])

    lane = iota((32, 128), 1)
    for c in range(2):
        total = brecv[4 * c].astype(F32)
        for m in range(1, 4):
            total = total + brecv[4 * c + m].astype(F32)
        rest = total[:, 512:640]
        for i in range(4):
            tail = rest if i == 0 else pltpu.roll(rest, 128 - 32 * i, 1)
            tail = jnp.where(lane < 32, tail, 0.0)
            wide = jnp.concatenate([total[:, 128 * i : 128 * i + 128], tail], axis=1)
            for h in range(2):
                pair = [wide[16 * p + 8 * h : 16 * p + 8 * h + 8] for p in range(2)]
                packed[h, pl.ds(16 * (4 * c + i), 16), :] = jnp.concatenate(pair, axis=0).astype(BF16)
    width = 8 * sensors
    compact = packed[...].reshape(256, 256)[:, 0:sensors]
    diagonal = iota((16, 256), 0) % 8 == iota((16, 256), 1) % 8
    for at in range(0, width, 256):
        size = min(256, width - at)
        spread = (iota((sensors, size), 0) == (at + iota((sensors, size), 1)) // 8).astype(BF16)
        spaced = jnp.dot(compact, spread, preferred_element_type=F32)
        for r in range(16):
            block = jnp.where(diagonal[:, 0:size], spaced[16 * r : 16 * r + 16], 0.0)
            rows = slice(16 * (r % 8), 16 * (r % 8) + 16)
            lhs_re[r // 8, rows, at : at + size] = block.astype(BF16)
            turned_block = jnp.concatenate([block[8:16], -block[0:8]], axis=0)
            lhs_im[r // 8, rows, at : at + size] = turned_block.astype(BF16)

    for copy in kernel_in:
        copy.wait()

    def lanes(tile, count=1):
        return slice(128 * tile, 128 * (tile + count))

    eighth = iota((8, 256), 0)
    weights = []
    for h in range(2):
        column = jnp.zeros((8, 256), F32)
        for k in range(8):
            column = jnp.where(eighth == k, prior_ref[8 * h + k] * (1.0 / 16.0), column)
        weights.append(column)

    for n, (left, right) in enumerate(CHUNKS):
        scale = jnp.concatenate([scale_ref[:, lanes(left)], scale_ref[:, lanes(right)]], axis=1)
        for h in range(2):
            product = jnp.zeros((128, 256), F32)
            for p, lhs in ((0, lhs_re), (1, lhs_im)):
                operand = jnp.concatenate(
                    [kern_v[h, p, :, :, lanes(left)], kern_v[h, p, :, :, lanes(right)]], axis=2
                ).reshape(width, 256)
                product = product + jnp.dot(lhs[h, :, 0:width], operand, preferred_element_type=F32)
            factor = jnp.concatenate([weights[h] * scale] * 4, axis=0)
            for d in range(4):
                zsend[n, d, pl.ds(32 * h, 32), :] = (product[32 * d : 32 * d + 32] * factor).astype(BF16)
        for o in range(1, 4):
            target = (s + o) % 4
            pltpu.make_async_remote_copy(
                zsend.at[n, target], zrecv.at[n, s], zsend_sem.at[n], zrecv_sem.at[n],
                device_id={"sens": target}, device_id_type=MESH,
            ).start()

    @pl.when(par == 0)
    def _():
        hrecv[0] = jnp.zeros((8, 128), F32)

    @pl.when(par == 3)
    def _():
        hrecv[1] = jnp.zeros((8, 128), F32)

    lane = iota((8, 128), 1)
    lane64 = iota((64, 128), 1)
    for n, (left, right) in enumerate(CHUNKS):
        drain(zrecv.at[n, pl.ds(0, 3)], zrecv_sem.at[n])
        total = zsend[n, s].astype(F32)
        for o in range(1, 4):
            total = total + zrecv[n, (s + o) % 4].astype(F32)
        zfull[:, lanes(left + 1)] = total[:, 0:128]
        zfull[:, lanes(right + 1)] = total[:, 128:256]
        if n == 0:
            for e, piece in ((0, total[:, 0:128]), (1, total[:, 128:256])):
                columns = jnp.zeros((8, 128), F32)
                for j in range(8):
                    shift = j + e
                    block = piece[8 * j : 8 * j + 8]
                    moved = block if shift == 0 else pltpu.roll(block, shift, 1)
                    columns = jnp.where(lane == j, moved, columns)
                hsend[e] = columns

            @pl.when(par > 0)
            def _():
                pltpu.make_async_remote_copy(
                    hsend.at[0], hrecv.at[1], hsend_sem.at[0], hrecv_sem.at[1],
                    device_id={"param": par - 1}, device_id_type=MESH,
                ).start()

            @pl.when(par < 3)
            def _():
                pltpu.make_async_remote_copy(
                    hsend.at[1], hrecv.at[0], hsend_sem.at[1], hrecv_sem.at[0],
                    device_id={"param": par + 1}, device_id_type=MESH,
                ).start()

        for t in READY[n]:
            if t == 0 or t == row - 1:
                e = 0 if t == 0 else 1

                @pl.when(par > 0 if e == 0 else par < 3)
                def _(e=e):
                    drain(hrecv.at[e], hrecv_sem.at[e])

                edge = hrecv[e]
                for j in range(8):
                    shift = 127 - j if e == 0 else (128 - j) % 128
                    moved = edge if shift == 0 else pltpu.roll(edge, shift, 1)
                    zfull[8 * j : 8 * j + 8, lanes(0 if e == 0 else row + 1)] = moved
            before, here, after = (zfull[:, lanes(t + i)] for i in range(3))
            low = jnp.where(lane64 == 0, pltpu.roll(before, 1, 1), pltpu.roll(here, 1, 1))
            high = jnp.where(lane64 == 127, pltpu.roll(after, 127, 1), pltpu.roll(here, 127, 1))
            smooth = (0.5 * here + 0.25 * (low + high)) * scale_ref[:, lanes(t)]
            for q in range(2):
                owner = 8 * q + t
                halves = [smooth[32 * h + 16 * q : 32 * h + 16 * q + 16] for h in range(2)]
                wsend[t, q] = jnp.concatenate(halves, axis=0).astype(BF16)
                piece = wsend.at[t, q]

                @pl.when(f != owner)
                def _(owner=owner, piece=piece):
                    pltpu.make_async_remote_copy(
                        piece, wrecv.at[f], send_sem.at[2], recv_sem.at[2],
                        device_id={"freq": owner}, device_id_type=MESH,
                    ).start()

                @pl.when(f == owner)
                def _(piece=piece):
                    pltpu.make_async_copy(piece, wrecv.at[f], recv_sem.at[2]).start()

    drain(wrecv, recv_sem.at[2])
    spectra = wrecv[...].reshape(512, 128)
    image = jnp.dot(table_hi[...], spectra, preferred_element_type=F32)
    image = image + jnp.dot(table_lo[...], spectra, preferred_element_type=F32)
    isend[...] = image.astype(BF16).reshape(16, 32, 128)
    for o in range(1, 16):
        target = (f + o) % 16
        pltpu.make_async_remote_copy(
            isend.at[target], irecv.at[f], send_sem.at[3], recv_sem.at[3],
            device_id={"freq": target}, device_id_type=MESH,
        ).start()
    irecv[f] = isend[f]

    drain(arecv.at[pl.ds(0, 3)], send_sem.at[0])
    drain(brecv.at[pl.ds(0, 7)], send_sem.at[1])
    for n in range(4):
        drain(zrecv.at[n, pl.ds(0, 3)], zsend_sem.at[n])

    @pl.when(par > 0)
    def _():
        drain(hsend.at[0], hsend_sem.at[0])

    @pl.when(par < 3)
    def _():
        drain(hsend.at[1], hsend_sem.at[1])

    drain(wrecv.at[pl.ds(0, 15)], send_sem.at[2])
    drain(isend.at[pl.ds(0, 15)], send_sem.at[3])
    drain(irecv.at[pl.ds(0, 15)], recv_sem.at[3])
    out_ref[...] = irecv[...]


def local(series, kern, prior_spectrum, prior_scale):
    sensors, params = kern.shape[2:]
    series, kern = series.transpose(2, 0, 1), kern.transpose(0, 2, 1, 3)
    vmem = pltpu.VMEM
    dma = pltpu.SemaphoreType.DMA
    image = pl.pallas_call(
        kernel,
        out_shape=jax.ShapeDtypeStruct((16, 32, 128), BF16),
        in_specs=[
            pl.BlockSpec(memory_space=pl.ANY),
            pl.BlockSpec(memory_space=pl.ANY),
            pl.BlockSpec(memory_space=pltpu.SMEM),
            pl.BlockSpec(memory_space=pltpu.VMEM),
        ],
        out_specs=pl.BlockSpec(memory_space=pltpu.VMEM),
        scratch_shapes=[
            vmem((26, 8, sensors), BF16),
            vmem((2, 2, sensors, 8, params), BF16),
            vmem((2, 208, 128), F32),
            vmem((32, 640), F32),
            vmem((4, 32, 640), BF16),
            vmem((4, 32, 640), BF16),
            vmem((8, 32, 640), BF16),
            vmem((2, 128, 256), BF16),
            vmem((2, 128, 8 * sensors), BF16),
            vmem((2, 128, 8 * sensors), BF16),
            vmem((4, 4, 64, 256), BF16),
            vmem((4, 4, 64, 256), BF16),
            vmem((64, 1280), F32),
            vmem((2, 8, 128), F32),
            vmem((2, 8, 128), F32),
            vmem((8, 2, 32, 128), BF16),
            vmem((16, 32, 128), BF16),
            vmem((16, 32, 128), BF16),
            vmem((16, 32, 128), BF16),
            vmem((512, 512), BF16),
            vmem((512, 512), BF16),
            dma((5,)),
            dma((4,)),
            dma((4,)),
            dma((4,)),
            dma((4,)),
            dma((2,)),
            dma((2,)),
        ],
        compiler_params=pltpu.CompilerParams(
            collective_id=0, has_side_effects=True, vmem_limit_bytes=60 * 1024 * 1024
        ),
        name="adjoint",
    )(series, kern, prior_spectrum, prior_scale.reshape(1, -1))
    image = image.reshape(2, 8, 32, 128)[:, :, :26].astype(F32)
    return image.transpose(2, 0, 1, 3).reshape(26, 2, params)


def solution(mesh):
    placed = (P(None, "sens", "freq"), P(None, "freq", "sens", "param"), P("freq"), P("param"))
    return jax.shard_map(
        local, mesh=mesh, in_specs=placed, out_specs=P("freq", "sens", "param"), check_vma=False
    )
```

```python
import functools
import math

import jax
import jax.numpy as jnp
from jax import lax
from jax.experimental import pallas as pl
from jax.experimental.pallas import tpu as pltpu
from jax.sharding import PartitionSpec as P

LEN = 840
MESH = pl.DeviceIdType.MESH
F32, BF16 = jnp.float32, jnp.bfloat16
CHUNKS = ((0, 7), (1, 2), (3, 4), (5, 6))
READY = ((), (0, 1), (2, 3), (4, 5, 6, 7))
STEPS = sorted(((i, j) for i in range(4) for j in range(4) if i + j), key=lambda v: -sum(min(a, 4 - a) for a in v))


def owner_of(half, tile):
    early, low = int(tile < 4), tile % 4
    at_y = 2 * half + low // 2
    return 4 * at_y + 2 * (low % 2) + (early + at_y) % 2


def iota(shape, dim):
    return lax.broadcasted_iota(jnp.int32, shape, dim)


def turned_cos(bins, times, part):
    turn = bins.astype(F32) * times.astype(F32) + (LEN // 4) * part.astype(F32)
    turn = turn - LEN * jnp.floor(turn * (1.0 / LEN) + 0.5)
    half = turn * (math.pi / LEN)
    square = half * half
    term = 1.0 / 6227020800.0
    for coef in (-1.0 / 39916800.0, 1.0 / 362880.0, -1.0 / 5040.0, 1.0 / 120.0, -1.0 / 6.0, 1.0):
        term = term * square + coef
    sine = half * term
    return 1.0 - 2.0 * sine * sine


def split(x):
    high = x.astype(BF16)
    return high, (x - high.astype(F32)).astype(BF16)


def kernel(
    series_ref, kern_ref, prior_hbm, scale_hbm, out_ref,
    prior_ref, scale_ref, ser_v, kern_v, by_time, turned, arecv, bsend, brecv, packed, lhs_re, lhs_im, zsend, zpart, zfwd, zrecv, zfull,
    hsend, hrecv, wsend, wrecv, isend, irecv, table_hi, table_lo,
    local_sem, send_sem, recv_sem, zsend_sem, zrecv_sem, hsend_sem, hrecv_sem,
):
    f, par, s = lax.axis_index("freq"), lax.axis_index("param"), lax.axis_index("sens")
    y, x = f // 4, f % 4
    core = par % 2
    sensors = ser_v.shape[2]
    row = kern_v.shape[4] // 128
    rest_of = sensors - 128
    late = 1 - (x + y) % 2
    slot = 8 * (y // 2) + 2 * (y % 2) + x // 2 + 4 * late
    end = (s == 0) | (s == 3)
    middle = (s == 1) | (s == 2)
    near, beyond = 1 + s // 3, 2 - s // 3
    across = 3 - s
    side = jnp.where(end, near, 3 * (s - 1))
    far = jnp.where(end, across, 6 - 3 * s)
    first_at = lambda j: j * (1 + 3 * core) + 4 * y * (1 - core) + x * core
    second_at = lambda m: m * (4 - 3 * core) + x * (1 - core) + 4 * y * core
    first_pos = x * (1 - core) + y * core
    second_pos = y * (1 - core) + x * core

    barrier = pltpu.get_barrier_semaphore()
    for i, j in sorted(STEPS, key=sum):
        peer = 4 * ((y + j) % 4) + (x + i) % 4
        pl.semaphore_signal(barrier, 1, device_id={"freq": peer}, device_id_type=MESH)
    for o in range(1, 4):
        pl.semaphore_signal(barrier, 1, device_id={"sens": (s + o) % 4}, device_id_type=MESH)
    other = par + 1 - 2 * core
    for m in range(4):
        source = m * (1 + 3 * core) + 4 * y * (1 - core) + x * core
        pl.semaphore_signal(barrier, 1, device_id={"freq": source, "param": other}, device_id_type=MESH)

    @pl.when(par == 1)
    def _():
        pl.semaphore_signal(barrier, 1, device_id={"param": 2}, device_id_type=MESH)

    @pl.when(par == 2)
    def _():
        pl.semaphore_signal(barrier, 1, device_id={"param": 1}, device_id_type=MESH)

    series_in = pltpu.make_async_copy(series_ref, ser_v, local_sem.at[0])
    series_in.start()
    small_in = []
    for n, (source, target) in enumerate(((prior_hbm, prior_ref), (scale_hbm, scale_ref))):
        small_in.append(pltpu.make_async_copy(source, target, local_sem.at[5 + n]))
        small_in[-1].start()
    kernel_in = []
    for p in range(2):
        for h in range(2):
            kernel_in.append(
                pltpu.make_async_copy(
                    kern_ref.at[p, :, pl.ds(8 * h, 8)], kern_v.at[h, p], local_sem.at[1 + 2 * h + p]
                )
            )
            kernel_in[-1].start()

    ri, ci = iota((128, 128), 0), iota((128, 128), 1)
    bins = 16 * second_at(ri >> 5) + (ri & 15)
    inside = ci & 31
    times = 26 * first_at(ci >> 5) + inside
    forward = jnp.where(inside < 26, turned_cos(bins, times, (ri >> 4) & 1), 0.0)
    fwd_hi, fwd_lo = split(forward)

    turned[:, 24:32, :] = jnp.zeros((2, 8, 384), F32)
    turned[:, :, 256:384] = jnp.zeros((2, 32, 128), F32)
    series_in.wait()
    by_time[0] = ser_v[:, :, 0:128].astype(F32).reshape(208, 128)
    by_time[1, :, 0:rest_of] = ser_v[:, :, 128:sensors].astype(F32).reshape(208, rest_of)
    for g in range(2):
        for q in range(2):
            rows = pl.ds((6 * core if g == 0 else 2 + 2 * core) + q, 26, stride=8)
            turned[g, 0:26, 128 * q : 128 * q + 128] = by_time[0, rows, :]
            turned[g, 0:26, 256 + 32 * q : 256 + 32 * q + rest_of] = by_time[1, rows, :][:, 0:rest_of]
        arecv[g, first_pos] = turned[g].astype(BF16)

    pl.semaphore_wait(barrier, 22 + jnp.where((par == 1) | (par == 2), 1, 0))

    for g in range(2):
        for o in (2, 1, 3):
            pltpu.make_async_remote_copy(
                arecv.at[g, first_pos], arecv.at[g, first_pos], send_sem.at[g], recv_sem.at[g],
                device_id={"freq": first_at((first_pos + o) % 4)}, device_id_type=MESH,
            ).start()

    @pl.loop(0, 16)
    def _(b):
        ti, ki = iota((32, 512), 0), iota((32, 512), 1)
        owner = 4 * ((y + 2 + b // 4) % 4) + b % 4
        values = turned_cos(((ki >> 5) << 4) + ((ki >> 4) & 1) * 8 + (ki & 7), 26 * owner + ti, (ki >> 3) & 1)
        high, low = split(values)
        rows = pl.ds(pl.multiple_of(32 * b, 32), 32)
        table_hi[rows, :] = high
        table_lo[rows, :] = low

    def drain(like, sem):
        pltpu.make_async_copy(like, like, sem).wait()

    for g in range(2):
        drain(arecv.at[g, pl.ds(0, 3)], recv_sem.at[g])
        gathered = arecv[g].reshape(128, 384)
        spec = jnp.dot(fwd_hi, gathered, preferred_element_type=F32)
        spec = spec + jnp.dot(fwd_lo, gathered, preferred_element_type=F32)
        spec = spec * (1.0 / math.sqrt(416.0))
        bsend[g] = spec.astype(BF16).reshape(4, 32, 384)
        for o in (2, 1, 3, 0):
            m = (second_pos + o) % 4
            for c in range(2):
                if o + c > 0:
                    target = par + (1 - 2 * core) * c
                    pltpu.make_async_remote_copy(
                        bsend.at[g, m], brecv.at[g, 4 * core + second_pos],
                        send_sem.at[2 + g], recv_sem.at[2 + g],
                        device_id={"freq": second_at(m), "param": target}, device_id_type=MESH,
                    ).start()
        brecv[g, 4 * core + second_pos] = bsend[g, second_pos]

    lane = iota((32, 128), 1)
    width = 8 * sensors
    diagonal = iota((16, 256), 0) % 8 == iota((16, 256), 1) % 8

    def spread_out(g):
        for c in range(2):
            total = brecv[g, 4 * c].astype(F32)
            for m in range(1, 4):
                total = total + brecv[g, 4 * c + m].astype(F32)
            for q in range(2):
                tail = total[:, 256:384]
                tail = tail if q == 0 else pltpu.roll(tail, 128 - 32 * q, 1)
                tail = jnp.where(lane < 32, tail, 0.0)
                wide = jnp.concatenate([total[:, 128 * q : 128 * q + 128], tail], axis=1)
                for h in range(2):
                    pair = [wide[16 * p + 8 * h : 16 * p + 8 * h + 8] for p in range(2)]
                    packed[g, h, pl.ds(32 * c + 16 * q, 16), :] = jnp.concatenate(pair, axis=0).astype(BF16)
        compact = packed[g].reshape(128, 256)[:, 0:sensors]
        for at in range(0, width, 256):
            size = min(256, width - at)
            spread = (iota((sensors, size), 0) == (at + iota((sensors, size), 1)) // 8).astype(BF16)
            spaced = jnp.dot(compact, spread, preferred_element_type=F32)
            for r in range(8):
                block = jnp.where(diagonal[:, 0:size], spaced[16 * r : 16 * r + 16], 0.0)
                rows = slice(16 * (r % 4), 16 * (r % 4) + 16)
                lhs_re[g, r // 4, rows, at : at + size] = block.astype(BF16)
                swapped = jnp.concatenate([block[8:16], -block[0:8]], axis=0)
                lhs_im[g, r // 4, rows, at : at + size] = swapped.astype(BF16)

    drain(brecv.at[0, pl.ds(0, 7)], recv_sem.at[2])
    spread_out(0)
    for copy in small_in + kernel_in:
        copy.wait()

    def send_along(source, target, kind, n, received, to):
        pltpu.make_async_remote_copy(
            source, target, zsend_sem.at[4 * kind + n], zrecv_sem.at[received],
            device_id={"sens": to}, device_id_type=MESH,
        ).start()

    def lanes(tile, count=1):
        return slice(128 * tile, 128 * (tile + count))

    eighth = iota((8, 256), 0)
    weights = []
    for h in range(2):
        column = jnp.zeros((8, 256), F32)
        for k in range(8):
            column = jnp.where(eighth == k, prior_ref[8 * h + k] * (1.0 / 16.0), column)
        weights.append(column)

    def contract(g, n):
        left, right = CHUNKS[n]
        scale = jnp.concatenate([scale_ref[:, lanes(left)], scale_ref[:, lanes(right)]], axis=1)
        for h in range(2):
            product = jnp.zeros((64, 256), F32)
            for p, lhs in ((0, lhs_re), (1, lhs_im)):
                operand = jnp.concatenate(
                    [kern_v[h, p, :, :, lanes(left)], kern_v[h, p, :, :, lanes(right)]], axis=2
                ).reshape(width, 256)
                product = product + jnp.dot(lhs[g, h, :, 0:width], operand, preferred_element_type=F32)
            factor = jnp.concatenate([weights[h] * scale] * 4, axis=0)
            for c, d in enumerate((1, 2) if g else (0, 3)):
                piece = product[32 * c : 32 * c + 32] * factor
                zpart[n, d, pl.ds(32 * h, 32), :] = piece
                zsend[n, d, pl.ds(32 * h, 32), :] = piece.astype(BF16)

    def pass_on(kind, n):
        @pl.when(middle)
        def _():
            drain(zrecv.at[n, 2 + kind], zrecv_sem.at[4 + 4 * kind + n])
            to = across if kind else far
            both = zpart[n, to] + zrecv[n, 2 + kind].astype(F32)
            zfwd[n, kind] = both.astype(BF16)
            send_along(zfwd.at[n, kind], zrecv.at[n, 1], 1 + kind, n, n, to)

    for n in range(4):
        contract(0, n)
        source, to = jnp.where(end, across, side), jnp.where(end, near, side)
        kind = jnp.where(end, 1, 0)
        send_along(zsend.at[n, source], zrecv.at[n, 2 * kind], 0, n, 4 * kind + n, to)
    drain(brecv.at[1, pl.ds(0, 7)], recv_sem.at[3])
    spread_out(1)
    for n in range(4):
        contract(1, n)

        @pl.when(end)
        def _(n=n):
            send_along(zsend.at[n, beyond], zrecv.at[n, 3], 1, n, 8 + n, near)

        if n == 1:
            pass_on(0, 0)
        if n == 2:
            pass_on(0, 1)

    def give_rest():
        for n in range(4):
            send_along(zsend.at[n, near], zrecv.at[n, 0], 2, n, n, near)

    pl.when(end)(give_rest)
    for kind, n in ((0, 2), (0, 3), (1, 0), (1, 1), (1, 2), (1, 3)):
        pass_on(kind, n)

    @pl.when(par == 0)
    def _():
        hrecv[0] = jnp.zeros((8, 128), F32)

    @pl.when(par == 3)
    def _():
        hrecv[1] = jnp.zeros((8, 128), F32)

    lane = iota((8, 128), 1)
    lane64 = iota((64, 128), 1)
    for n, (left, right) in enumerate(CHUNKS):
        drain(zrecv.at[n, pl.ds(0, 2)], zrecv_sem.at[n])
        total = zpart[n, s] + zrecv[n, 0].astype(F32) + zrecv[n, 1].astype(F32)
        zfull[:, lanes(left + 1)] = total[:, 0:128]
        zfull[:, lanes(right + 1)] = total[:, 128:256]
        if n == 0:
            for e, piece in ((0, total[:, 0:128]), (1, total[:, 128:256])):
                columns = jnp.zeros((8, 128), F32)
                for j in range(8):
                    shift = j + e
                    block = piece[8 * j : 8 * j + 8]
                    moved = block if shift == 0 else pltpu.roll(block, shift, 1)
                    columns = jnp.where(lane == j, moved, columns)
                hsend[e] = columns

            @pl.when(par > 0)
            def _():
                pltpu.make_async_remote_copy(
                    hsend.at[0], hrecv.at[1], hsend_sem.at[0], hrecv_sem.at[1],
                    device_id={"param": par - 1}, device_id_type=MESH,
                ).start()

            @pl.when(par < 3)
            def _():
                pltpu.make_async_remote_copy(
                    hsend.at[1], hrecv.at[0], hsend_sem.at[1], hrecv_sem.at[0],
                    device_id={"param": par + 1}, device_id_type=MESH,
                ).start()

        for t in READY[n]:
            if t == 0 or t == row - 1:
                e = 0 if t == 0 else 1

                @pl.when(par > 0 if e == 0 else par < 3)
                def _(e=e):
                    drain(hrecv.at[e], hrecv_sem.at[e])

                edge = hrecv[e]
                for j in range(8):
                    shift = 127 - j if e == 0 else (128 - j) % 128
                    moved = edge if shift == 0 else pltpu.roll(edge, shift, 1)
                    zfull[8 * j : 8 * j + 8, lanes(0 if e == 0 else row + 1)] = moved
            before, here, after = (zfull[:, lanes(t + i)] for i in range(3))
            low = jnp.where(lane64 == 0, pltpu.roll(before, 1, 1), pltpu.roll(here, 1, 1))
            high = jnp.where(lane64 == 127, pltpu.roll(after, 127, 1), pltpu.roll(here, 127, 1))
            smooth = (0.5 * here + 0.25 * (low + high)) * scale_ref[:, lanes(t)]
            for q in range(2):
                owner = owner_of(q, t)
                halves = [smooth[32 * h + 16 * q : 32 * h + 16 * q + 16] for h in range(2)]
                wsend[t, q] = jnp.concatenate(halves, axis=0).astype(BF16)
                piece = wsend.at[t, q]

                @pl.when(f != owner)
                def _(owner=owner, piece=piece):
                    pltpu.make_async_remote_copy(
                        piece, wrecv.at[f], send_sem.at[4], recv_sem.at[4],
                        device_id={"freq": owner}, device_id_type=MESH,
                    ).start()

                @pl.when(f == owner)
                def _(piece=piece):
                    pltpu.make_async_copy(piece, wrecv.at[f], recv_sem.at[4]).start()

    drain(wrecv, recv_sem.at[4])
    spectra = wrecv[...].reshape(512, 128)
    for half in range(2):
        rows = slice(256 * half, 256 * half + 256)
        image = jnp.dot(table_hi[rows, :], spectra, preferred_element_type=F32)
        image = image + jnp.dot(table_lo[rows, :], spectra, preferred_element_type=F32)
        isend[8 * half : 8 * half + 8] = image.astype(BF16).reshape(8, 32, 128)
        for j in (0, 1) if half == 0 else (3, 2):
            row_y = (y + 2 + j) % 4
            for i in (2, 1, 3, 0):
                if i > 0 or j != 2:
                    target_x = (x + i) % 4
                    pltpu.make_async_remote_copy(
                        isend.at[4 * j + target_x], irecv.at[slot], send_sem.at[5], recv_sem.at[5 + late],
                        device_id={"freq": 4 * row_y + target_x}, device_id_type=MESH,
                    ).start()
    pltpu.make_async_copy(isend.at[8 + x], irecv.at[slot], recv_sem.at[5 + late]).start()

    for g in range(2):
        drain(arecv.at[g, pl.ds(0, 3)], send_sem.at[g])
        drain(brecv.at[g, pl.ds(0, 7)], send_sem.at[2 + g])
    for n in range(12):
        drain(zfwd.at[0, 0], zsend_sem.at[n])

    @pl.when(par > 0)
    def _():
        drain(hsend.at[0], hsend_sem.at[0])

    @pl.when(par < 3)
    def _():
        drain(hsend.at[1], hsend_sem.at[1])

    drain(wrecv.at[pl.ds(0, 15)], send_sem.at[4])
    drain(isend.at[pl.ds(0, 15)], send_sem.at[5])
    for last in range(2):
        drain(irecv.at[pl.ds(0, 8)], recv_sem.at[5 + last])
        for q in range(2):
            for t in range(4 * last, 4 * last + 4):
                out_ref[pl.ds(2 * t + q, 26, stride=16), :] = irecv[8 * q + t, 0:26, :].astype(F32)


def local(series, kern, prior_spectrum, prior_scale):
    sensors, params = kern.shape[2:]
    series, kern = series.transpose(2, 0, 1), kern.transpose(0, 2, 1, 3)
    vmem = pltpu.VMEM
    dma = pltpu.SemaphoreType.DMA
    operands = (series, kern, prior_spectrum, prior_scale.reshape(1, -1))
    image = pl.pallas_call(
        kernel,
        out_shape=jax.ShapeDtypeStruct((416, 128), F32),
        in_specs=[
            pl.BlockSpec(memory_space=pl.ANY),
        ] * 4,
        out_specs=pl.BlockSpec(memory_space=pltpu.VMEM),
        scratch_shapes=[
            pltpu.SMEM((16,), F32),
            vmem((1, params), F32),
            vmem((26, 8, sensors), BF16),
            vmem((2, 2, sensors, 8, params), BF16),
            vmem((2, 208, 128), F32),
            vmem((2, 32, 384), F32),
            vmem((2, 4, 32, 384), BF16),
            vmem((2, 4, 32, 384), BF16),
            vmem((2, 8, 32, 384), BF16),
            vmem((2, 2, 64, 256), BF16),
            vmem((2, 2, 64, 8 * sensors), BF16),
            vmem((2, 2, 64, 8 * sensors), BF16),
            vmem((4, 4, 64, 256), BF16),
            vmem((4, 4, 64, 256), F32),
            vmem((4, 2, 64, 256), BF16),
            vmem((4, 4, 64, 256), BF16),
            vmem((64, 1280), F32),
            vmem((2, 8, 128), F32),
            vmem((2, 8, 128), F32),
            vmem((8, 2, 32, 128), BF16),
            vmem((16, 32, 128), BF16),
            vmem((16, 32, 128), BF16),
            vmem((16, 32, 128), BF16),
            vmem((512, 512), BF16),
            vmem((512, 512), BF16),
            dma((7,)),
            dma((6,)),
            dma((7,)),
            dma((12,)),
            dma((12,)),
            dma((2,)),
            dma((2,)),
        ],
        compiler_params=pltpu.CompilerParams(
            collective_id=0, has_side_effects=True, vmem_limit_bytes=50 * 1024 * 1024
        ),
        name="adjoint",
    )(*(pltpu.with_memory_space_constraint(v, pltpu.HBM) for v in operands))
    return image.reshape(26, 8, 2, 128).transpose(0, 2, 1, 3).reshape(26, 2, params)


def solution(mesh):
    placed = (P(None, "sens", "freq"), P(None, "freq", "sens", "param"), P("freq"), P("param"))
    return jax.shard_map(
        local, mesh=mesh, in_specs=placed, out_specs=P("freq", "sens", "param"), check_vma=False
    )
```

```python
import functools
import math

import jax
import jax.numpy as jnp
from jax import lax
from jax.experimental import pallas as pl
from jax.experimental.pallas import tpu as pltpu
from jax.sharding import PartitionSpec as P

LEN = 840
MESH = pl.DeviceIdType.MESH
F32, BF16 = jnp.float32, jnp.bfloat16
CHUNKS = ((0, 7), (1, 2), (3, 4), (5, 6))
READY = ((), (1,), (2, 3, 0), (4, 5, 6, 7))
STEPS = sorted(((i, j) for i in range(4) for j in range(4) if i + j), key=lambda v: -sum(min(a, 4 - a) for a in v))


def owner_of(half, tile):
    early, low = int(tile < 4), tile % 4
    at_y = 2 * half + low // 2
    return 4 * at_y + 2 * (low % 2) + (early + at_y) % 2


def iota(shape, dim):
    return lax.broadcasted_iota(jnp.int32, shape, dim)


def turned_cos(bins, times, part):
    turn = bins.astype(F32) * times.astype(F32) + (LEN // 4) * part.astype(F32)
    turn = turn - LEN * jnp.floor(turn * (1.0 / LEN) + 0.5)
    half = turn * (math.pi / LEN)
    square = half * half
    term = 1.0 / 6227020800.0
    for coef in (-1.0 / 39916800.0, 1.0 / 362880.0, -1.0 / 5040.0, 1.0 / 120.0, -1.0 / 6.0, 1.0):
        term = term * square + coef
    sine = half * term
    return 1.0 - 2.0 * sine * sine


def split(x):
    high = x.astype(BF16)
    return high, (x - high.astype(F32)).astype(BF16)


def kernel(
    series_ref, kern_ref, prior_hbm, scale_hbm, out_ref,
    prior_ref, scale_ref, ser_v, kern_v, by_time, turned, arecv, bsend, brecv, packed, lhs_re, lhs_im, zsend, zpart, zfwd, zrecv, zfull,
    hsend, hrecv, wsend, wrecv, isend, irecv, table_hi, table_lo,
    local_sem, send_sem, recv_sem, zsend_sem, zrecv_sem, hsend_sem, hrecv_sem, round_sem,
):
    f, par, s = lax.axis_index("freq"), lax.axis_index("param"), lax.axis_index("sens")
    y, x = f // 4, f % 4
    core = par % 2
    sensors = ser_v.shape[2]
    row = kern_v.shape[4] // 128
    rest_of = sensors - 128
    late = 1 - (x + y) % 2
    slot = 8 * (y // 2) + 2 * (y % 2) + x // 2 + 4 * late
    end = (s == 0) | (s == 3)
    middle = (s == 1) | (s == 2)
    near, beyond = 1 + s // 3, 2 - s // 3
    across = 3 - s
    side = jnp.where(end, near, 3 * (s - 1))
    far = jnp.where(end, across, 6 - 3 * s)
    first_at = lambda j: j * (1 + 3 * core) + 4 * y * (1 - core) + x * core
    second_at = lambda m: m * (4 - 3 * core) + x * (1 - core) + 4 * y * core
    first_pos = x * (1 - core) + y * core
    second_pos = y * (1 - core) + x * core

    barrier = pltpu.get_barrier_semaphore()
    other = par + 1 - 2 * core
    in_plane = [{"freq": first_at((first_pos + o) % 4)} for o in (2, 1, 3)] + [{"param": other}]

    def greet(sem, peers):
        for peer in peers:
            pl.semaphore_signal(sem, 1, device_id=peer, device_id_type=MESH)

    greet(barrier, in_plane)
    for o in range(1, 4):

        @pl.when(s + o < 4)
        def _(o=o):
            greet(barrier, [{"sens": s + o}, {"sens": s + o, "param": other}])

    @pl.when(par == 1)
    def _():
        greet(barrier, [{"sens": d, "param": 2} for d in range(4)])

    series_in = pltpu.make_async_copy(series_ref, ser_v, local_sem.at[0])
    series_in.start()
    small_in = []
    for n, (source, target) in enumerate(((prior_hbm, prior_ref), (scale_hbm, scale_ref))):
        small_in.append(pltpu.make_async_copy(source, target, local_sem.at[5 + n]))
        small_in[-1].start()
    kernel_in = []
    for p in range(2):
        for h in range(2):
            kernel_in.append(
                pltpu.make_async_copy(
                    kern_ref.at[p, :, pl.ds(8 * h, 8)], kern_v.at[h, p], local_sem.at[1 + 2 * h + p]
                )
            )
            kernel_in[-1].start()

    ri, ci = iota((128, 128), 0), iota((128, 128), 1)
    bins = 16 * second_at(ri >> 5) + (ri & 15)
    inside = ci & 31
    times = 26 * first_at(ci >> 5) + inside
    forward = jnp.where(inside < 26, turned_cos(bins, times, (ri >> 4) & 1), 0.0)
    fwd_hi, fwd_lo = split(forward)

    turned[:, 24:32, :] = jnp.zeros((2, 8, 384), F32)
    turned[:, :, 256:384] = jnp.zeros((2, 32, 128), F32)
    series_in.wait()
    by_time[0] = ser_v[:, :, 0:128].astype(F32).reshape(208, 128)
    by_time[1, :, 0:rest_of] = ser_v[:, :, 128:sensors].astype(F32).reshape(208, rest_of)
    for g in range(2):
        for q in range(2):
            rows = pl.ds((6 * core if g == 0 else 2 + 2 * core) + q, 26, stride=8)
            turned[g, 0:26, 128 * q : 128 * q + 128] = by_time[0, rows, :]
            turned[g, 0:26, 256 + 32 * q : 256 + 32 * q + rest_of] = by_time[1, rows, :][:, 0:rest_of]
        arecv[g, first_pos] = turned[g].astype(BF16)

    pl.semaphore_wait(barrier, 4 + 2 * s + jnp.where(par == 2, 4, 0))

    for g in range(2):
        for o in (2, 1, 3):
            pltpu.make_async_remote_copy(
                arecv.at[g, first_pos], arecv.at[g, first_pos], send_sem.at[g], recv_sem.at[g],
                device_id={"freq": first_at((first_pos + o) % 4)}, device_id_type=MESH,
            ).start()

    greet(round_sem.at[0], in_plane)

    for o in range(1, 4):

        @pl.when(s >= o)
        def _(o=o):
            greet(round_sem.at[2], [{"sens": s - o}])
            greet(round_sem.at[3], [{"sens": s - o, "param": other}])

    @pl.when(par == 2)
    def _():
        greet(round_sem.at[3], [{"sens": d, "param": 1} for d in range(4)])

    @pl.loop(0, 16)
    def _(b):
        ti, ki = iota((32, 512), 0), iota((32, 512), 1)
        owner = 4 * ((y + 2 + b // 4) % 4) + b % 4
        values = turned_cos(((ki >> 5) << 4) + ((ki >> 4) & 1) * 8 + (ki & 7), 26 * owner + ti, (ki >> 3) & 1)
        high, low = split(values)
        rows = pl.ds(pl.multiple_of(32 * b, 32), 32)
        table_hi[rows, :] = high
        table_lo[rows, :] = low

    def drain(like, sem):
        pltpu.make_async_copy(like, like, sem).wait()

    pl.semaphore_wait(round_sem.at[0], 4)
    greet(round_sem.at[1], in_plane)
    for g in range(2):
        drain(arecv.at[g, pl.ds(0, 3)], recv_sem.at[g])
        gathered = arecv[g].reshape(128, 384)
        spec = jnp.dot(fwd_hi, gathered, preferred_element_type=F32)
        spec = spec + jnp.dot(fwd_lo, gathered, preferred_element_type=F32)
        spec = spec * (1.0 / math.sqrt(416.0))
        bsend[g] = spec.astype(BF16).reshape(4, 32, 384)
        if g == 0:
            pl.semaphore_wait(round_sem.at[1], 4)
        for o in (2, 1, 3, 0):
            m = (second_pos + o) % 4
            for c in range(2):
                if o + c > 0:
                    target = par + (1 - 2 * core) * c
                    pltpu.make_async_remote_copy(
                        bsend.at[g, m], brecv.at[g, 4 * core + second_pos],
                        send_sem.at[2 + g], recv_sem.at[2 + g],
                        device_id={"freq": second_at(m), "param": target}, device_id_type=MESH,
                    ).start()
        brecv[g, 4 * core + second_pos] = bsend[g, second_pos]

    lane = iota((32, 128), 1)
    width = 8 * sensors
    diagonal = iota((16, 256), 0) % 8 == iota((16, 256), 1) % 8

    def spread_out(g):
        for c in range(2):
            total = brecv[g, 4 * c].astype(F32)
            for m in range(1, 4):
                total = total + brecv[g, 4 * c + m].astype(F32)
            for q in range(2):
                tail = total[:, 256:384]
                tail = tail if q == 0 else pltpu.roll(tail, 128 - 32 * q, 1)
                tail = jnp.where(lane < 32, tail, 0.0)
                wide = jnp.concatenate([total[:, 128 * q : 128 * q + 128], tail], axis=1)
                for h in range(2):
                    pair = [wide[16 * p + 8 * h : 16 * p + 8 * h + 8] for p in range(2)]
                    packed[g, h, pl.ds(32 * c + 16 * q, 16), :] = jnp.concatenate(pair, axis=0).astype(BF16)
        compact = packed[g].reshape(128, 256)[:, 0:sensors]
        for at in range(0, width, 256):
            size = min(256, width - at)
            spread = (iota((sensors, size), 0) == (at + iota((sensors, size), 1)) // 8).astype(BF16)
            spaced = jnp.dot(compact, spread, preferred_element_type=F32)
            for r in range(8):
                block = jnp.where(diagonal[:, 0:size], spaced[16 * r : 16 * r + 16], 0.0)
                rows = slice(16 * (r % 4), 16 * (r % 4) + 16)
                lhs_re[g, r // 4, rows, at : at + size] = block.astype(BF16)
                swapped = jnp.concatenate([block[8:16], -block[0:8]], axis=0)
                lhs_im[g, r // 4, rows, at : at + size] = swapped.astype(BF16)

    drain(brecv.at[0, pl.ds(0, 7)], recv_sem.at[2])
    spread_out(0)
    for copy in small_in + kernel_in:
        copy.wait()

    @pl.when(s < 3)
    def _():
        pl.semaphore_wait(round_sem.at[2], 3 - s)


    def send_along(source, target, kind, n, received, to):
        pltpu.make_async_remote_copy(
            source, target, zsend_sem.at[4 * kind + n], zrecv_sem.at[received],
            device_id={"sens": to}, device_id_type=MESH,
        ).start()

    def lanes(tile, count=1):
        return slice(128 * tile, 128 * (tile + count))

    eighth = iota((8, 256), 0)
    weights = []
    for h in range(2):
        column = jnp.zeros((8, 256), F32)
        for k in range(8):
            column = jnp.where(eighth == k, prior_ref[8 * h + k] * (1.0 / 16.0), column)
        weights.append(column)

    def lead(n):
        source, to = jnp.where(end, across, side), jnp.where(end, near, side)
        kind = jnp.where(end, 1, 0)
        send_along(zsend.at[n, source], zrecv.at[n, 2 * kind], 0, n, 4 * kind + n, to)

    def contract(g, n):
        left, right = CHUNKS[n]
        scale = jnp.concatenate([scale_ref[:, lanes(left)], scale_ref[:, lanes(right)]], axis=1)
        for h in range(2):
            product = jnp.zeros((64, 256), F32)
            for p, lhs in ((0, lhs_re), (1, lhs_im)):
                operand = jnp.concatenate(
                    [kern_v[h, p, :, :, lanes(left)], kern_v[h, p, :, :, lanes(right)]], axis=2
                ).reshape(width, 256)
                product = product + jnp.dot(lhs[g, h, :, 0:width], operand, preferred_element_type=F32)
            factor = jnp.concatenate([weights[h] * scale] * 4, axis=0)
            for c, d in enumerate((1, 2) if g else (0, 3)):
                piece = product[32 * c : 32 * c + 32] * factor
                zpart[n, d, pl.ds(32 * h, 32), :] = piece
                zsend[n, d, pl.ds(32 * h, 32), :] = piece.astype(BF16)

    def pass_on(kind, n):
        @pl.when(middle)
        def _():
            drain(zrecv.at[n, 2 + kind], zrecv_sem.at[4 + 4 * kind + n])
            to = across if kind else far
            both = zpart[n, to] + zrecv[n, 2 + kind].astype(F32)
            zfwd[n, kind] = both.astype(BF16)
            send_along(zfwd.at[n, kind], zrecv.at[n, 1], 1 + kind, n, n, to)

    lane8 = iota((8, 128), 1)

    @pl.when(par == 0)
    def _():
        hrecv[0] = jnp.zeros((4, 8, 128), BF16)

    @pl.when(par == 3)
    def _():
        hrecv[1] = jnp.zeros((4, 8, 128), BF16)

    def send_edges(g):
        for d in (1, 2) if g else (0, 3):
            for e in range(2):
                columns = jnp.zeros((8, 128), F32)
                for j in range(8):
                    block = zpart[0, d, 8 * j : 8 * j + 8, lanes(e)]
                    moved = block if j + e == 0 else pltpu.roll(block, j + e, 1)
                    columns = jnp.where(lane8 == j, moved, columns)
                hsend[e, d] = columns.astype(BF16)

        @pl.when(par > 0)
        def _():
            for d in (1, 2) if g else (0, 3):
                pltpu.make_async_remote_copy(
                    hsend.at[0, d], hrecv.at[1, s], hsend_sem.at[0], hrecv_sem.at[1],
                    device_id={"param": par - 1, "sens": d}, device_id_type=MESH,
                ).start()

        @pl.when(par < 3)
        def _():
            for d in (1, 2) if g else (0, 3):
                pltpu.make_async_remote_copy(
                    hsend.at[1, d], hrecv.at[0, s], hsend_sem.at[1], hrecv_sem.at[0],
                    device_id={"param": par + 1, "sens": d}, device_id_type=MESH,
                ).start()

    for n in range(4):
        contract(0, n)
        lead(n)
    drain(brecv.at[1, pl.ds(0, 7)], recv_sem.at[3])
    spread_out(1)
    for n in range(4):
        contract(1, n)

        @pl.when(end)
        def _(n=n):
            send_along(zsend.at[n, beyond], zrecv.at[n, 3], 1, n, 8 + n, near)

        if n == 0:

            @pl.when((s < 3) | (par == 1))
            def _():
                pl.semaphore_wait(round_sem.at[3], 3 - s + jnp.where(par == 1, 4, 0))

            send_edges(0)
            send_edges(1)
        if n == 1:
            pass_on(0, 0)
        if n == 2:
            pass_on(0, 1)

    def give_rest():
        for n in range(4):
            send_along(zsend.at[n, near], zrecv.at[n, 0], 2, n, n, near)

    pl.when(end)(give_rest)
    for kind, n in ((0, 2), (0, 3), (1, 0), (1, 1), (1, 2), (1, 3)):
        pass_on(kind, n)

    lane64 = iota((64, 128), 1)
    for n, (left, right) in enumerate(CHUNKS):
        drain(zrecv.at[n, pl.ds(0, 2)], zrecv_sem.at[n])
        total = zpart[n, s] + zrecv[n, 0].astype(F32) + zrecv[n, 1].astype(F32)
        zfull[:, lanes(left + 1)] = total[:, 0:128]
        zfull[:, lanes(right + 1)] = total[:, 128:256]
        for t in READY[n]:
            if t == 0 or t == row - 1:
                e = 0 if t == 0 else 1

                @pl.when(par > 0 if e == 0 else par < 3)
                def _(e=e):
                    drain(hrecv.at[e], hrecv_sem.at[e])

                edge = hrecv[e, 0].astype(F32)
                for o in range(1, 4):
                    edge = edge + hrecv[e, o].astype(F32)
                for j in range(8):
                    shift = 127 - j if e == 0 else (128 - j) % 128
                    moved = edge if shift == 0 else pltpu.roll(edge, shift, 1)
                    zfull[8 * j : 8 * j + 8, lanes(0 if e == 0 else row + 1)] = moved
            before, here, after = (zfull[:, lanes(t + i)] for i in range(3))
            low = jnp.where(lane64 == 0, pltpu.roll(before, 1, 1), pltpu.roll(here, 1, 1))
            high = jnp.where(lane64 == 127, pltpu.roll(after, 127, 1), pltpu.roll(here, 127, 1))
            smooth = (0.5 * here + 0.25 * (low + high)) * scale_ref[:, lanes(t)]
            for q in range(2):
                owner = owner_of(q, t)
                halves = [smooth[32 * h + 16 * q : 32 * h + 16 * q + 16] for h in range(2)]
                wsend[t, q] = jnp.concatenate(halves, axis=0).astype(BF16)
                piece = wsend.at[t, q]

                @pl.when(f != owner)
                def _(owner=owner, piece=piece):
                    pltpu.make_async_remote_copy(
                        piece, wrecv.at[f], send_sem.at[4], recv_sem.at[4],
                        device_id={"freq": owner}, device_id_type=MESH,
                    ).start()

                @pl.when(f == owner)
                def _(piece=piece):
                    pltpu.make_async_copy(piece, wrecv.at[f], recv_sem.at[4]).start()

    drain(wrecv, recv_sem.at[4])
    spectra = wrecv[...].reshape(512, 128)
    for half in range(2):
        rows = slice(256 * half, 256 * half + 256)
        image = jnp.dot(table_hi[rows, :], spectra, preferred_element_type=F32)
        image = image + jnp.dot(table_lo[rows, :], spectra, preferred_element_type=F32)
        isend[8 * half : 8 * half + 8] = image.astype(BF16).reshape(8, 32, 128)
        for j in (0, 1) if half == 0 else (3, 2):
            row_y = (y + 2 + j) % 4
            for i in (2, 1, 3, 0):
                if i > 0 or j != 2:
                    target_x = (x + i) % 4
                    pltpu.make_async_remote_copy(
                        isend.at[4 * j + target_x], irecv.at[slot], send_sem.at[5], recv_sem.at[5 + late],
                        device_id={"freq": 4 * row_y + target_x}, device_id_type=MESH,
                    ).start()
    pltpu.make_async_copy(isend.at[8 + x], irecv.at[slot], recv_sem.at[5 + late]).start()

    for g in range(2):
        drain(arecv.at[g, pl.ds(0, 3)], send_sem.at[g])
        drain(brecv.at[g, pl.ds(0, 7)], send_sem.at[2 + g])
    for n in range(12):
        drain(zfwd.at[0, 0], zsend_sem.at[n])

    @pl.when(par > 0)
    def _():
        drain(hsend.at[0], hsend_sem.at[0])

    @pl.when(par < 3)
    def _():
        drain(hsend.at[1], hsend_sem.at[1])

    drain(wrecv.at[pl.ds(0, 15)], send_sem.at[4])
    drain(isend.at[pl.ds(0, 15)], send_sem.at[5])
    for last in range(2):
        drain(irecv.at[pl.ds(0, 8)], recv_sem.at[5 + last])
        for q in range(2):
            for t in range(4 * last, 4 * last + 4):
                out_ref[pl.ds(2 * t + q, 26, stride=16), :] = irecv[8 * q + t, 0:26, :].astype(F32)


def local(series, kern, prior_spectrum, prior_scale):
    sensors, params = kern.shape[2:]
    series, kern = series.transpose(2, 0, 1), kern.transpose(0, 2, 1, 3)
    vmem = pltpu.VMEM
    dma = pltpu.SemaphoreType.DMA
    operands = (series, kern, prior_spectrum, prior_scale.reshape(1, -1))
    image = pl.pallas_call(
        kernel,
        out_shape=jax.ShapeDtypeStruct((416, 128), F32),
        in_specs=[
            pl.BlockSpec(memory_space=pl.ANY),
        ] * 4,
        out_specs=pl.BlockSpec(memory_space=pltpu.VMEM),
        scratch_shapes=[
            pltpu.SMEM((16,), F32),
            vmem((1, params), F32),
            vmem((26, 8, sensors), BF16),
            vmem((2, 2, sensors, 8, params), BF16),
            vmem((2, 208, 128), F32),
            vmem((2, 32, 384), F32),
            vmem((2, 4, 32, 384), BF16),
            vmem((2, 4, 32, 384), BF16),
            vmem((2, 8, 32, 384), BF16),
            vmem((2, 2, 64, 256), BF16),
            vmem((2, 2, 64, 8 * sensors), BF16),
            vmem((2, 2, 64, 8 * sensors), BF16),
            vmem((4, 4, 64, 256), BF16),
            vmem((4, 4, 64, 256), F32),
            vmem((4, 2, 64, 256), BF16),
            vmem((4, 4, 64, 256), BF16),
            vmem((64, 1280), F32),
            vmem((2, 4, 8, 128), BF16),
            vmem((2, 4, 8, 128), BF16),
            vmem((8, 2, 32, 128), BF16),
            vmem((16, 32, 128), BF16),
            vmem((16, 32, 128), BF16),
            vmem((16, 32, 128), BF16),
            vmem((512, 512), BF16),
            vmem((512, 512), BF16),
            dma((7,)),
            dma((6,)),
            dma((7,)),
            dma((12,)),
            dma((12,)),
            dma((2,)),
            dma((2,)),
            pltpu.SemaphoreType.REGULAR((4,)),
        ],
        compiler_params=pltpu.CompilerParams(
            collective_id=0, has_side_effects=True, vmem_limit_bytes=50 * 1024 * 1024
        ),
        name="adjoint",
    )(*(pltpu.with_memory_space_constraint(v, pltpu.HBM) for v in operands))
    return image.reshape(26, 8, 2, 128).transpose(0, 2, 1, 3).reshape(26, 2, params)


def solution(mesh):
    placed = (P(None, "sens", "freq"), P(None, "freq", "sens", "param"), P("freq"), P("param"))
    return jax.shard_map(
        local, mesh=mesh, in_specs=placed, out_specs=P("freq", "sens", "param"), check_vma=False
    )
```

```python
import functools
import math

import jax
import jax.numpy as jnp
from jax import lax
from jax.experimental import pallas as pl
from jax.experimental.pallas import tpu as pltpu
from jax.sharding import PartitionSpec as P

LEN = 840
MESH = pl.DeviceIdType.MESH
F32, BF16 = jnp.float32, jnp.bfloat16
CHUNKS = ((0, 7), (1, 2), (3, 4), (5, 6))
READY = ((), (), (0, 1, 2, 3), (4, 5, 6, 7))
STEPS = sorted(((i, j) for i in range(4) for j in range(4) if i + j), key=lambda v: -sum(min(a, 4 - a) for a in v))


def iota(shape, dim):
    return lax.broadcasted_iota(jnp.int32, shape, dim)


def turned_cos(bins, times, part):
    turn = bins.astype(F32) * times.astype(F32) + (LEN // 4) * part.astype(F32)
    turn = turn - LEN * jnp.floor(turn * (1.0 / LEN) + 0.5)
    half = turn * (math.pi / LEN)
    square = half * half
    term = 1.0 / 6227020800.0
    for coef in (-1.0 / 39916800.0, 1.0 / 362880.0, -1.0 / 5040.0, 1.0 / 120.0, -1.0 / 6.0, 1.0):
        term = term * square + coef
    sine = half * term
    return 1.0 - 2.0 * sine * sine


def split(x):
    high = x.astype(BF16)
    return high, (x - high.astype(F32)).astype(BF16)


def kernel(
    series_ref, kern_ref, prior_hbm, scale_hbm, out_ref,
    prior_ref, scale_ref, ser_v, kern_v, by_time, turned, arecv, bsend, brecv, packed, lhs_re, lhs_im, zsend, zpart, zfwd, zrecv, zfull,
    hsend, hrecv, wsend, wrecv, isend, irecv, out_v, table_hi, table_lo,
    local_sem, send_sem, recv_sem, zsend_sem, zrecv_sem, hsend_sem, hrecv_sem, round_sem,
):
    f, par, s = lax.axis_index("freq"), lax.axis_index("param"), lax.axis_index("sens")
    y, x = f // 4, f % 4
    core = par % 2
    sensors = ser_v.shape[2]
    row = kern_v.shape[4] // 128
    rest_of = sensors - 128
    late = 1 - (x + y) % 2
    slot = 8 * (y // 2) + 2 * (y % 2) + x // 2 + 4 * late
    end = (s == 0) | (s == 3)
    middle = (s == 1) | (s == 2)
    near, beyond = 1 + s // 3, 2 - s // 3
    across = 3 - s
    side = jnp.where(end, near, 3 * (s - 1))
    far = jnp.where(end, across, 6 - 3 * s)
    first_at = lambda j: j * (1 + 3 * core) + 4 * y * (1 - core) + x * core
    second_at = lambda m: m * (4 - 3 * core) + x * (1 - core) + 4 * y * core
    first_pos = x * (1 - core) + y * core
    second_pos = y * (1 - core) + x * core

    series_in = pltpu.make_async_copy(series_ref, ser_v, local_sem.at[0])
    series_in.start()
    barrier = pltpu.get_barrier_semaphore()
    other = par + 1 - 2 * core
    in_plane = [{"freq": first_at((first_pos + o) % 4)} for o in (2, 1, 3)] + [{"param": other}]

    def greet(sem, peers):
        for peer in peers:
            pl.semaphore_signal(sem, 1, device_id=peer, device_id_type=MESH)

    greet(barrier, in_plane)
    for o in range(1, 4):

        @pl.when(s + o < 4)
        def _(o=o):
            greet(barrier, [{"sens": s + o}, {"sens": s + o, "param": other}])

    @pl.when(par == 1)
    def _():
        greet(barrier, [{"sens": d, "param": 2} for d in range(4)])

    small_in = []
    for n, (source, target) in enumerate(((prior_hbm, prior_ref), (scale_hbm, scale_ref))):
        small_in.append(pltpu.make_async_copy(source, target, local_sem.at[5 + n]))
        small_in[-1].start()
    kernel_in = []
    for p in range(2):
        for h in range(2):
            kernel_in.append(
                pltpu.make_async_copy(
                    kern_ref.at[p, :, pl.ds(8 * h, 8)], kern_v.at[h, p], local_sem.at[1 + 2 * h + p]
                )
            )
            kernel_in[-1].start()

    ri, ci = iota((128, 128), 0), iota((128, 128), 1)
    bins = 16 * second_at(ri >> 5) + (ri & 15)
    inside = ci & 31
    times = 26 * first_at(ci >> 5) + inside
    forward = jnp.where(inside < 26, turned_cos(bins, times, (ri >> 4) & 1), 0.0)
    fwd_hi, fwd_lo = split(forward)

    turned[:, 24:32, :] = jnp.zeros((2, 8, 384), F32)
    turned[:, :, 256:384] = jnp.zeros((2, 32, 128), F32)
    series_in.wait()
    by_time[0] = ser_v[:, :, 0:128].astype(F32).reshape(208, 128)
    by_time[1, :, 0:rest_of] = ser_v[:, :, 128:sensors].astype(F32).reshape(208, rest_of)
    for g in range(2):
        for q in range(2):
            rows = pl.ds((6 * core if g == 0 else 2 + 2 * core) + q, 26, stride=8)
            turned[g, 0:26, 128 * q : 128 * q + 128] = by_time[0, rows, :]
            turned[g, 0:26, 256 + 32 * q : 256 + 32 * q + rest_of] = by_time[1, rows, :][:, 0:rest_of]
        arecv[g, first_pos] = turned[g].astype(BF16)

    pl.semaphore_wait(barrier, 4 + 2 * s + jnp.where(par == 2, 4, 0))

    for g in range(2):
        for o in (2, 1, 3):
            pltpu.make_async_remote_copy(
                arecv.at[g, first_pos], arecv.at[g, first_pos], send_sem.at[g], recv_sem.at[g],
                device_id={"freq": first_at((first_pos + o) % 4)}, device_id_type=MESH,
            ).start()

    greet(round_sem.at[0], in_plane)

    for o in range(1, 4):

        @pl.when(s >= o)
        def _(o=o):
            greet(round_sem.at[2], [{"sens": s - o}])
            greet(round_sem.at[3], [{"sens": s - o, "param": other}])

    @pl.when(par == 2)
    def _():
        greet(round_sem.at[3], [{"sens": d, "param": 1} for d in range(4)])

    @pl.loop(0, 16)
    def _(b):
        ti, ki = iota((32, 512), 0), iota((32, 512), 1)
        owner = 4 * ((y + 2 + b // 4) % 4) + b % 4
        values = turned_cos(((ki >> 5) << 4) + ((ki >> 4) & 1) * 8 + (ki & 7), 26 * owner + ti, (ki >> 3) & 1)
        high, low = split(values)
        rows = pl.ds(pl.multiple_of(32 * b, 32), 32)
        table_hi[rows, :] = high
        table_lo[rows, :] = low

    def drain(like, sem):
        pltpu.make_async_copy(like, like, sem).wait()

    pl.semaphore_wait(round_sem.at[0], 4)
    greet(round_sem.at[1], in_plane)
    for g in range(2):
        drain(arecv.at[g, pl.ds(0, 3)], recv_sem.at[g])
        gathered = arecv[g].reshape(128, 384)
        spec = jnp.dot(fwd_hi, gathered, preferred_element_type=F32)
        spec = spec + jnp.dot(fwd_lo, gathered, preferred_element_type=F32)
        spec = spec * (1.0 / math.sqrt(416.0))
        bsend[g] = spec.astype(BF16).reshape(4, 32, 384)
        if g == 0:
            pl.semaphore_wait(round_sem.at[1], 4)
        for o in (2, 1, 3, 0):
            m = (second_pos + o) % 4
            for c in range(2):
                if o + c > 0:
                    target = par + (1 - 2 * core) * c
                    pltpu.make_async_remote_copy(
                        bsend.at[g, m], brecv.at[g, 4 * core + second_pos],
                        send_sem.at[2 + g], recv_sem.at[2 + g],
                        device_id={"freq": second_at(m), "param": target}, device_id_type=MESH,
                    ).start()
        brecv[g, 4 * core + second_pos] = bsend[g, second_pos]

    lane = iota((32, 128), 1)
    width = 8 * sensors
    diagonal = iota((16, 256), 0) % 8 == iota((16, 256), 1) % 8

    def spread_out(g):
        for c in range(2):
            total = brecv[g, 4 * c].astype(F32)
            for m in range(1, 4):
                total = total + brecv[g, 4 * c + m].astype(F32)
            for q in range(2):
                tail = total[:, 256:384]
                tail = tail if q == 0 else pltpu.roll(tail, 128 - 32 * q, 1)
                tail = jnp.where(lane < 32, tail, 0.0)
                wide = jnp.concatenate([total[:, 128 * q : 128 * q + 128], tail], axis=1)
                for h in range(2):
                    pair = [wide[16 * p + 8 * h : 16 * p + 8 * h + 8] for p in range(2)]
                    packed[g, h, pl.ds(32 * c + 16 * q, 16), :] = jnp.concatenate(pair, axis=0).astype(BF16)
        compact = packed[g].reshape(128, 256)[:, 0:sensors]
        for at in range(0, width, 256):
            size = min(256, width - at)
            spread = (iota((sensors, size), 0) == (at + iota((sensors, size), 1)) // 8).astype(BF16)
            spaced = jnp.dot(compact, spread, preferred_element_type=F32)
            for r in range(8):
                block = jnp.where(diagonal[:, 0:size], spaced[16 * r : 16 * r + 16], 0.0)
                rows = slice(16 * (r % 4), 16 * (r % 4) + 16)
                lhs_re[g, r // 4, rows, at : at + size] = block.astype(BF16)
                swapped = jnp.concatenate([block[8:16], -block[0:8]], axis=0)
                lhs_im[g, r // 4, rows, at : at + size] = swapped.astype(BF16)

    drain(brecv.at[0, pl.ds(0, 7)], recv_sem.at[2])
    spread_out(0)
    for copy in small_in + kernel_in:
        copy.wait()

    @pl.when(s < 3)
    def _():
        pl.semaphore_wait(round_sem.at[2], 3 - s)


    def send_along(source, target, kind, n, received, to):
        pltpu.make_async_remote_copy(
            source, target, zsend_sem.at[4 * kind + n], zrecv_sem.at[received],
            device_id={"sens": to}, device_id_type=MESH,
        ).start()

    def lanes(tile, count=1):
        return slice(128 * tile, 128 * (tile + count))

    eighth = iota((8, 256), 0)
    weights = []
    for h in range(2):
        column = jnp.zeros((8, 256), F32)
        for k in range(8):
            column = jnp.where(eighth == k, prior_ref[8 * h + k] * (1.0 / 16.0), column)
        weights.append(column)

    def lead(n):
        source, to = jnp.where(end, across, side), jnp.where(end, near, side)
        kind = jnp.where(end, 1, 0)
        send_along(zsend.at[n, source], zrecv.at[n, 2 * kind], 0, n, 4 * kind + n, to)

    def contract(g, n):
        left, right = CHUNKS[n]
        scale = jnp.concatenate([scale_ref[:, lanes(left)], scale_ref[:, lanes(right)]], axis=1)
        for h in range(2):
            product = jnp.zeros((64, 256), F32)
            for p, lhs in ((0, lhs_re), (1, lhs_im)):
                operand = jnp.concatenate(
                    [kern_v[h, p, :, :, lanes(left)], kern_v[h, p, :, :, lanes(right)]], axis=2
                ).reshape(width, 256)
                product = product + jnp.dot(lhs[g, h, :, 0:width], operand, preferred_element_type=F32)
            factor = jnp.concatenate([weights[h] * scale] * 4, axis=0)
            for c, d in enumerate((1, 2) if g else (0, 3)):
                piece = product[32 * c : 32 * c + 32] * factor
                zpart[n, d, pl.ds(32 * h, 32), :] = piece
                zsend[n, d, pl.ds(32 * h, 32), :] = piece.astype(BF16)

    def parts_of(kind, n):
        return (pl.ds(0, 32), pl.ds(32, 32)) if kind == 1 and n == 3 else (pl.ds(0, 64),)

    def pass_on(kind, n):
        @pl.when(middle)
        def _():
            to = across if kind else far
            for m, part in enumerate(parts_of(kind, n)):
                drain(zrecv.at[n, 2 + kind, part], zrecv_sem.at[12 if m else 4 + 4 * kind + n])
                both = zpart[n, to, part] + zrecv[n, 2 + kind, part].astype(F32)
                zfwd[n, kind, part] = both.astype(BF16)
                send_along(zfwd.at[n, kind, part], zrecv.at[n, 1, part], 1 + kind, n, n, to)

    lane8 = iota((8, 128), 1)

    @pl.when(par == 0)
    def _():
        hrecv[0] = jnp.zeros((4, 8, 128), BF16)

    @pl.when(par == 3)
    def _():
        hrecv[1] = jnp.zeros((4, 8, 128), BF16)

    def send_edges(g):
        for d in (1, 2) if g else (0, 3):
            for e in range(2):
                columns = jnp.zeros((8, 128), F32)
                for j in range(8):
                    block = zpart[0, d, 8 * j : 8 * j + 8, lanes(e)]
                    moved = block if j + e == 0 else pltpu.roll(block, j + e, 1)
                    columns = jnp.where(lane8 == j, moved, columns)
                hsend[e, d] = columns.astype(BF16)

        @pl.when(par > 0)
        def _():
            for d in (1, 2) if g else (0, 3):
                pltpu.make_async_remote_copy(
                    hsend.at[0, d], hrecv.at[1, s], hsend_sem.at[0], hrecv_sem.at[1],
                    device_id={"param": par - 1, "sens": d}, device_id_type=MESH,
                ).start()

        @pl.when(par < 3)
        def _():
            for d in (1, 2) if g else (0, 3):
                pltpu.make_async_remote_copy(
                    hsend.at[1, d], hrecv.at[0, s], hsend_sem.at[1], hrecv_sem.at[0],
                    device_id={"param": par + 1, "sens": d}, device_id_type=MESH,
                ).start()

    for n in range(4):
        contract(0, n)
        lead(n)
    drain(brecv.at[1, pl.ds(0, 7)], recv_sem.at[3])
    spread_out(1)
    for n in range(4):
        contract(1, n)

        @pl.when(end)
        def _(n=n):
            for m, part in enumerate(parts_of(1, n)):
                send_along(zsend.at[n, beyond, part], zrecv.at[n, 3, part], 1, n, 12 if m else 8 + n, near)

        if n == 0:

            @pl.when((s < 3) | (par == 1))
            def _():
                pl.semaphore_wait(round_sem.at[3], 3 - s + jnp.where(par == 1, 4, 0))

            send_edges(0)
            send_edges(1)
        if n == 1:
            pass_on(0, 0)
        if n == 2:
            pass_on(0, 1)

    def give_rest():
        for n in range(4):
            send_along(zsend.at[n, near], zrecv.at[n, 0], 2, n, n, near)

    pl.when(end)(give_rest)
    for kind, n in ((0, 2), (0, 3), (1, 0), (1, 1), (1, 2), (1, 3)):
        pass_on(kind, n)

    lane64 = iota((64, 128), 1)
    for n, (left, right) in enumerate(CHUNKS):
        drain(zrecv.at[n, pl.ds(0, 2)], zrecv_sem.at[n])
        total = zpart[n, s] + zrecv[n, 0].astype(F32) + zrecv[n, 1].astype(F32)
        zfull[:, lanes(left + 1)] = total[:, 0:128]
        zfull[:, lanes(right + 1)] = total[:, 128:256]
        for e, t in ((0, 0), (1, row - 1)):
            if t in READY[n]:

                @pl.when(par > 0 if e == 0 else par < 3)
                def _(e=e):
                    drain(hrecv.at[e], hrecv_sem.at[e])

                edge = hrecv[e, 0].astype(F32)
                for o in range(1, 4):
                    edge = edge + hrecv[e, o].astype(F32)
                for j in range(8):
                    shift = 127 - j if e == 0 else (128 - j) % 128
                    moved = edge if shift == 0 else pltpu.roll(edge, shift, 1)
                    zfull[8 * j : 8 * j + 8, lanes(0 if e == 0 else row + 1)] = moved
        for t in READY[n]:
            before, here, after = (zfull[:, lanes(t + i)] for i in range(3))
            low = jnp.where(lane64 == 0, pltpu.roll(before, 1, 1), pltpu.roll(here, 1, 1))
            high = jnp.where(lane64 == 127, pltpu.roll(after, 127, 1), pltpu.roll(here, 127, 1))
            smooth = (0.5 * here + 0.25 * (low + high)) * scale_ref[:, lanes(t)]
            for q in range(2):
                halves = [smooth[32 * h + 16 * q : 32 * h + 16 * q + 16] for h in range(2)]
                wsend[t, q] = jnp.concatenate(halves, axis=0).astype(BF16)
        if n >= 2:
            upper = n - 2
            for mine in range(2):

                @pl.when(late == mine)
                def _(upper=upper, mine=mine):
                    for i, j in STEPS:
                        if (i + j + mine + upper) % 2 == 0:
                            to_y, to_x = (y + j) % 4, (x + i) % 4
                            t = 4 * upper + 2 * (to_y % 2) + to_x // 2
                            pltpu.make_async_remote_copy(
                                wsend.at[t, to_y // 2], wrecv.at[f], send_sem.at[4], recv_sem.at[4],
                                device_id={"freq": 4 * to_y + to_x}, device_id_type=MESH,
                            ).start()
                    if mine == upper:
                        own = wsend.at[4 * upper + 2 * (y % 2) + x // 2, y // 2]
                        pltpu.make_async_copy(own, wrecv.at[f], recv_sem.at[4]).start()

    drain(wrecv, recv_sem.at[4])
    spectra = wrecv[...].reshape(512, 128)
    for half in range(2):
        rows = slice(256 * half, 256 * half + 256)
        image = jnp.dot(table_hi[rows, :], spectra, preferred_element_type=F32)
        image = image + jnp.dot(table_lo[rows, :], spectra, preferred_element_type=F32)
        isend[8 * half : 8 * half + 8] = image.astype(BF16).reshape(8, 32, 128)
        for j in (0, 1) if half == 0 else (3, 2):
            row_y = (y + 2 + j) % 4
            for i in (2, 1, 3, 0):
                if i > 0 or j != 2:
                    target_x = (x + i) % 4
                    pltpu.make_async_remote_copy(
                        isend.at[4 * j + target_x], irecv.at[slot], send_sem.at[5], recv_sem.at[5 + late],
                        device_id={"freq": 4 * row_y + target_x}, device_id_type=MESH,
                    ).start()
    pltpu.make_async_copy(isend.at[8 + x], irecv.at[slot], recv_sem.at[5 + late]).start()

    for g in range(2):
        drain(arecv.at[g, pl.ds(0, 3)], send_sem.at[g])
        drain(brecv.at[g, pl.ds(0, 7)], send_sem.at[2 + g])
    for n in range(12):
        drain(zfwd.at[0, 0], zsend_sem.at[n])

    @pl.when(par > 0)
    def _():
        drain(hsend.at[0], hsend_sem.at[0])

    @pl.when(par < 3)
    def _():
        drain(hsend.at[1], hsend_sem.at[1])

    drain(wrecv.at[pl.ds(0, 15)], send_sem.at[4])
    drain(isend.at[pl.ds(0, 15)], send_sem.at[5])
    out_copies = []
    for last in range(2):
        drain(irecv.at[pl.ds(0, 8)], recv_sem.at[5 + last])
        for q in range(2):
            for t in range(4):
                piece = irecv[8 * q + 4 * last + t, 0:26, :].astype(F32)
                out_v[last, pl.ds(2 * t + q, 26, stride=8), :] = piece
        out_copies.append(
            pltpu.make_async_copy(
                out_v.at[last].reshape(26, 8, 128), out_ref.at[:, pl.ds(8 * last, 8)], local_sem.at[last]
            )
        )
        out_copies[-1].start()
    for copy in out_copies:
        copy.wait()


def local(series, kern, prior_spectrum, prior_scale):
    sensors, params = kern.shape[2:]
    series, kern = series.transpose(2, 0, 1), kern.transpose(0, 2, 1, 3)
    vmem = pltpu.VMEM
    dma = pltpu.SemaphoreType.DMA
    operands = (series, kern, prior_spectrum, prior_scale.reshape(1, -1))
    image = pl.pallas_call(
        kernel,
        out_shape=jax.ShapeDtypeStruct((26, 16, 128), F32),
        in_specs=[
            pl.BlockSpec(memory_space=pl.ANY),
        ] * 4,
        out_specs=pl.BlockSpec(memory_space=pl.ANY),
        scratch_shapes=[
            pltpu.SMEM((16,), F32),
            vmem((1, params), F32),
            vmem((26, 8, sensors), BF16),
            vmem((2, 2, sensors, 8, params), BF16),
            vmem((2, 208, 128), F32),
            vmem((2, 32, 384), F32),
            vmem((2, 4, 32, 384), BF16),
            vmem((2, 4, 32, 384), BF16),
            vmem((2, 8, 32, 384), BF16),
            vmem((2, 2, 64, 256), BF16),
            vmem((2, 2, 64, 8 * sensors), BF16),
            vmem((2, 2, 64, 8 * sensors), BF16),
            vmem((4, 4, 64, 256), BF16),
            vmem((4, 4, 64, 256), F32),
            vmem((4, 2, 64, 256), BF16),
            vmem((4, 4, 64, 256), BF16),
            vmem((64, 1280), F32),
            vmem((2, 4, 8, 128), BF16),
            vmem((2, 4, 8, 128), BF16),
            vmem((8, 2, 32, 128), BF16),
            vmem((16, 32, 128), BF16),
            vmem((16, 32, 128), BF16),
            vmem((16, 32, 128), BF16),
            vmem((2, 208, 128), F32),
            vmem((512, 512), BF16),
            vmem((512, 512), BF16),
            dma((7,)),
            dma((6,)),
            dma((7,)),
            dma((12,)),
            dma((13,)),
            dma((2,)),
            dma((2,)),
            pltpu.SemaphoreType.REGULAR((4,)),
        ],
        compiler_params=pltpu.CompilerParams(
            collective_id=0, has_side_effects=True, vmem_limit_bytes=50 * 1024 * 1024
        ),
        name="adjoint",
    )(*(pltpu.with_memory_space_constraint(v, pltpu.HBM) for v in operands))
    return image.reshape(26, 8, 2, 128).transpose(0, 2, 1, 3).reshape(26, 2, params)


def solution(mesh):
    placed = (P(None, "sens", "freq"), P(None, "freq", "sens", "param"), P("freq"), P("param"))
    return jax.shard_map(
        local, mesh=mesh, in_specs=placed, out_specs=P("freq", "sens", "param"), check_vma=False
    )
```

```python
import functools
import math

import jax
import jax.numpy as jnp
from jax import lax
from jax.experimental import pallas as pl
from jax.experimental.pallas import tpu as pltpu
from jax.sharding import PartitionSpec as P

LEN = 840
MESH = pl.DeviceIdType.MESH
F32, BF16 = jnp.float32, jnp.bfloat16
CHUNKS = ((0, 7), (1, 2), (3, 4), (5, 6))
READY = ((), (), (0, 1, 2, 3), (4, 5, 6, 7))
STEPS = sorted(((i, j) for i in range(4) for j in range(4) if i + j), key=lambda v: -sum(min(a, 4 - a) for a in v))


def iota(shape, dim):
    return lax.broadcasted_iota(jnp.int32, shape, dim)


def turned_cos(bins, times, part):
    turn = bins.astype(F32) * times.astype(F32) + (LEN // 4) * part.astype(F32)
    turn = turn - LEN * jnp.floor(turn * (1.0 / LEN) + 0.5)
    half = turn * (math.pi / LEN)
    square = half * half
    term = 1.0 / 6227020800.0
    for coef in (-1.0 / 39916800.0, 1.0 / 362880.0, -1.0 / 5040.0, 1.0 / 120.0, -1.0 / 6.0, 1.0):
        term = term * square + coef
    sine = half * term
    return 1.0 - 2.0 * sine * sine


def split(x):
    high = x.astype(BF16)
    return high, (x - high.astype(F32)).astype(BF16)


def kernel(
    series_ref, kern_ref, prior_hbm, scale_hbm, out_ref,
    prior_ref, scale_ref, ser_v, kern_v, by_time, turned, arecv, bsend, brecv, packed, lhs_re, lhs_im, zsend, zpart, zfwd, zrecv, zfull,
    hsend, hrecv, wsend, wrecv, isend, irecv, out_v, table_hi, table_lo,
    local_sem, send_sem, recv_sem, zsend_sem, zrecv_sem, hsend_sem, hrecv_sem, round_sem,
):
    f, par, s = lax.axis_index("freq"), lax.axis_index("param"), lax.axis_index("sens")
    y, x = f // 4, f % 4
    core = par % 2
    sensors = ser_v.shape[2]
    row = kern_v.shape[4] // 128
    rest_of = sensors - 128
    late = 1 - (x + y) % 2
    slot = 8 * (y // 2) + 2 * (y % 2) + x // 2 + 4 * late
    end = (s == 0) | (s == 3)
    middle = (s == 1) | (s == 2)
    near, beyond = 1 + s // 3, 2 - s // 3
    across = 3 - s
    side = jnp.where(end, near, 3 * (s - 1))
    far = jnp.where(end, across, 6 - 3 * s)
    first_at = lambda j: j * (1 + 3 * core) + 4 * y * (1 - core) + x * core
    second_at = lambda m: m * (4 - 3 * core) + x * (1 - core) + 4 * y * core
    first_pos = x * (1 - core) + y * core
    second_pos = y * (1 - core) + x * core

    series_in = pltpu.make_async_copy(series_ref, ser_v, local_sem.at[0])
    series_in.start()
    barrier = pltpu.get_barrier_semaphore()
    other = par + 1 - 2 * core
    in_plane = [{"freq": first_at((first_pos + o) % 4)} for o in (2, 1, 3)] + [{"param": other}]

    def greet(sem, peers):
        for peer in peers:
            pl.semaphore_signal(sem, 1, device_id=peer, device_id_type=MESH)

    greet(barrier, in_plane)
    for o in range(1, 4):

        @pl.when(s + o < 4)
        def _(o=o):
            greet(barrier, [{"sens": s + o}, {"sens": s + o, "param": other}])

    @pl.when(par == 1)
    def _():
        greet(barrier, [{"sens": d, "param": 2} for d in range(4)])

    small_in = []
    for n, (source, target) in enumerate(((prior_hbm, prior_ref), (scale_hbm, scale_ref))):
        small_in.append(pltpu.make_async_copy(source, target, local_sem.at[5 + n]))
        small_in[-1].start()
    kernel_in = []
    for p in range(2):
        for h in range(2):
            kernel_in.append(
                pltpu.make_async_copy(
                    kern_ref.at[p, :, pl.ds(8 * h, 8)], kern_v.at[h, p], local_sem.at[1 + 2 * h + p]
                )
            )
            kernel_in[-1].start()

    ri, ci = iota((128, 128), 0), iota((128, 128), 1)
    bins = 16 * second_at(ri >> 5) + (ri & 15)
    inside = ci & 31
    times = 26 * first_at(ci >> 5) + inside
    forward = jnp.where(inside < 26, turned_cos(bins, times, (ri >> 4) & 1), 0.0)
    fwd_hi, fwd_lo = split(forward)

    turned[:, 24:32, :] = jnp.zeros((2, 8, 384), F32)
    turned[:, :, 256:384] = jnp.zeros((2, 32, 128), F32)
    series_in.wait()
    by_time[0, 0:208, :] = ser_v[:, :, 0:128].astype(F32).reshape(208, 128)
    by_time[1, 0:208, 0:rest_of] = ser_v[:, :, 128:sensors].astype(F32).reshape(208, rest_of)
    for g in range(2):
        for q in range(2):
            rows = pl.ds((6 * core if g == 0 else 2 + 2 * core) + q, 26, stride=8)
            turned[g, 0:26, 128 * q : 128 * q + 128] = by_time[0, rows, :]
            turned[g, 0:26, 256 + 32 * q : 256 + 32 * q + rest_of] = by_time[1, rows, :][:, 0:rest_of]
        arecv[g, first_pos] = turned[g].astype(BF16)

    pl.semaphore_wait(barrier, 4 + 2 * s + jnp.where(par == 2, 4, 0))

    for g in range(2):
        for o in (2, 1, 3):
            pltpu.make_async_remote_copy(
                arecv.at[g, first_pos], arecv.at[g, first_pos], send_sem.at[g], recv_sem.at[g],
                device_id={"freq": first_at((first_pos + o) % 4)}, device_id_type=MESH,
            ).start()

    greet(round_sem.at[0], in_plane)

    for o in range(1, 4):

        @pl.when(s >= o)
        def _(o=o):
            greet(round_sem.at[2], [{"sens": s - o}])
            greet(round_sem.at[3], [{"sens": s - o, "param": other}])

    @pl.when(par == 2)
    def _():
        greet(round_sem.at[3], [{"sens": d, "param": 1} for d in range(4)])

    @pl.loop(0, 16)
    def _(b):
        ti, ki = iota((32, 512), 0), iota((32, 512), 1)
        owner = 4 * ((y + 2 + b // 4) % 4) + b % 4
        values = turned_cos(((ki >> 5) << 4) + ((ki >> 4) & 1) * 8 + (ki & 7), 26 * owner + ti, (ki >> 3) & 1)
        high, low = split(values)
        rows = pl.ds(pl.multiple_of(32 * b, 32), 32)
        table_hi[rows, :] = high
        table_lo[rows, :] = low

    def drain(like, sem):
        pltpu.make_async_copy(like, like, sem).wait()

    pl.semaphore_wait(round_sem.at[0], 4)
    greet(round_sem.at[1], in_plane)
    for g in range(2):
        drain(arecv.at[g, pl.ds(0, 3)], recv_sem.at[g])
        gathered = arecv[g].reshape(128, 384)
        spec = jnp.dot(fwd_hi, gathered, preferred_element_type=F32)
        spec = spec + jnp.dot(fwd_lo, gathered, preferred_element_type=F32)
        spec = spec * (1.0 / math.sqrt(416.0))
        bsend[g] = spec.astype(BF16).reshape(4, 32, 384)
        if g == 0:
            pl.semaphore_wait(round_sem.at[1], 4)
        for o in (2, 1, 3, 0):
            m = (second_pos + o) % 4
            for c in range(2):
                if o + c > 0:
                    target = par + (1 - 2 * core) * c
                    pltpu.make_async_remote_copy(
                        bsend.at[g, m], brecv.at[g, 4 * core + second_pos],
                        send_sem.at[2 + g], recv_sem.at[2 + g],
                        device_id={"freq": second_at(m), "param": target}, device_id_type=MESH,
                    ).start()
        brecv[g, 4 * core + second_pos] = bsend[g, second_pos]

    lane = iota((32, 128), 1)
    width = 8 * sensors
    diagonal = iota((16, 256), 0) % 8 == iota((16, 256), 1) % 8

    def spread_out(g):
        for c in range(2):
            total = brecv[g, 4 * c].astype(F32)
            for m in range(1, 4):
                total = total + brecv[g, 4 * c + m].astype(F32)
            for q in range(2):
                tail = total[:, 256:384]
                tail = tail if q == 0 else pltpu.roll(tail, 128 - 32 * q, 1)
                tail = jnp.where(lane < 32, tail, 0.0)
                wide = jnp.concatenate([total[:, 128 * q : 128 * q + 128], tail], axis=1)
                for h in range(2):
                    pair = [wide[16 * p + 8 * h : 16 * p + 8 * h + 8] for p in range(2)]
                    packed[g, h, pl.ds(32 * c + 16 * q, 16), :] = jnp.concatenate(pair, axis=0).astype(BF16)
        compact = packed[g].reshape(128, 256)[:, 0:sensors]
        for at in range(0, width, 256):
            size = min(256, width - at)
            spread = (iota((sensors, size), 0) == (at + iota((sensors, size), 1)) // 8).astype(BF16)
            spaced = jnp.dot(compact, spread, preferred_element_type=F32)
            for r in range(8):
                block = jnp.where(diagonal[:, 0:size], spaced[16 * r : 16 * r + 16], 0.0)
                rows = slice(16 * (r % 4), 16 * (r % 4) + 16)
                lhs_re[g, r // 4, rows, at : at + size] = block.astype(BF16)
                swapped = jnp.concatenate([block[8:16], -block[0:8]], axis=0)
                lhs_im[g, r // 4, rows, at : at + size] = swapped.astype(BF16)

    drain(brecv.at[0, pl.ds(0, 7)], recv_sem.at[2])
    spread_out(0)
    for copy in small_in + kernel_in:
        copy.wait()

    @pl.when(s < 3)
    def _():
        pl.semaphore_wait(round_sem.at[2], 3 - s)


    def send_along(source, target, kind, n, received, to):
        pltpu.make_async_remote_copy(
            source, target, zsend_sem.at[4 * kind + n], zrecv_sem.at[received],
            device_id={"sens": to}, device_id_type=MESH,
        ).start()

    def lanes(tile, count=1):
        return slice(128 * tile, 128 * (tile + count))

    eighth = iota((8, 256), 0)
    weights = []
    for h in range(2):
        column = jnp.zeros((8, 256), F32)
        for k in range(8):
            column = jnp.where(eighth == k, prior_ref[8 * h + k] * (1.0 / 16.0), column)
        weights.append(column)

    def lead(n):
        source, to = jnp.where(end, across, side), jnp.where(end, near, side)
        kind = jnp.where(end, 1, 0)
        send_along(zsend.at[n, source], zrecv.at[n, 2 * kind], 0, n, 4 * kind + n, to)

    def contract(g, n):
        left, right = CHUNKS[n]
        scale = jnp.concatenate([scale_ref[:, lanes(left)], scale_ref[:, lanes(right)]], axis=1)
        for h in range(2):
            product = jnp.zeros((64, 256), F32)
            for p, lhs in ((0, lhs_re), (1, lhs_im)):
                operand = jnp.concatenate(
                    [kern_v[h, p, :, :, lanes(left)], kern_v[h, p, :, :, lanes(right)]], axis=2
                ).reshape(width, 256)
                product = product + jnp.dot(lhs[g, h, :, 0:width], operand, preferred_element_type=F32)
            factor = jnp.concatenate([weights[h] * scale] * 4, axis=0)
            for c, d in enumerate((1, 2) if g else (0, 3)):
                piece = product[32 * c : 32 * c + 32] * factor
                zpart[n, d, pl.ds(32 * h, 32), :] = piece
                zsend[n, d, pl.ds(32 * h, 32), :] = piece.astype(BF16)

    def parts_of(kind, n):
        return (pl.ds(0, 32), pl.ds(32, 32)) if kind == 1 and n == 3 else (pl.ds(0, 64),)

    def pass_on(kind, n):
        @pl.when(middle)
        def _():
            to = across if kind else far
            for m, part in enumerate(parts_of(kind, n)):
                drain(zrecv.at[n, 2 + kind, part], zrecv_sem.at[12 if m else 4 + 4 * kind + n])
                both = zpart[n, to, part] + zrecv[n, 2 + kind, part].astype(F32)
                zfwd[n, kind, part] = both.astype(BF16)
                send_along(zfwd.at[n, kind, part], zrecv.at[n, 1, part], 1 + kind, n, n, to)

    lane8 = iota((8, 128), 1)

    @pl.when(par == 0)
    def _():
        hrecv[0] = jnp.zeros((4, 8, 128), BF16)

    @pl.when(par == 3)
    def _():
        hrecv[1] = jnp.zeros((4, 8, 128), BF16)

    def send_edges(g):
        for d in (1, 2) if g else (0, 3):
            for e in range(2):
                columns = jnp.zeros((8, 128), F32)
                for j in range(8):
                    block = zpart[0, d, 8 * j : 8 * j + 8, lanes(e)]
                    moved = block if j + e == 0 else pltpu.roll(block, j + e, 1)
                    columns = jnp.where(lane8 == j, moved, columns)
                hsend[e, d] = columns.astype(BF16)

        @pl.when(par > 0)
        def _():
            for d in (1, 2) if g else (0, 3):
                pltpu.make_async_remote_copy(
                    hsend.at[0, d], hrecv.at[1, s], hsend_sem.at[0], hrecv_sem.at[1],
                    device_id={"param": par - 1, "sens": d}, device_id_type=MESH,
                ).start()

        @pl.when(par < 3)
        def _():
            for d in (1, 2) if g else (0, 3):
                pltpu.make_async_remote_copy(
                    hsend.at[1, d], hrecv.at[0, s], hsend_sem.at[1], hrecv_sem.at[0],
                    device_id={"param": par + 1, "sens": d}, device_id_type=MESH,
                ).start()

    for n in range(4):
        contract(0, n)
        lead(n)
    drain(brecv.at[1, pl.ds(0, 7)], recv_sem.at[3])
    spread_out(1)
    for n in range(4):
        contract(1, n)

        @pl.when(end)
        def _(n=n):
            for m, part in enumerate(parts_of(1, n)):
                send_along(zsend.at[n, beyond, part], zrecv.at[n, 3, part], 1, n, 12 if m else 8 + n, near)

        if n == 0:

            @pl.when((s < 3) | (par == 1))
            def _():
                pl.semaphore_wait(round_sem.at[3], 3 - s + jnp.where(par == 1, 4, 0))

            send_edges(0)
            send_edges(1)
        if n == 1:
            pass_on(0, 0)
        if n == 2:
            pass_on(0, 1)

    def give_rest():
        for n in range(4):
            send_along(zsend.at[n, near], zrecv.at[n, 0], 2, n, n, near)

    pl.when(end)(give_rest)
    for kind, n in ((0, 2), (0, 3), (1, 0), (1, 1), (1, 2), (1, 3)):
        pass_on(kind, n)

    lane64 = iota((64, 128), 1)
    for n, (left, right) in enumerate(CHUNKS):
        drain(zrecv.at[n, pl.ds(0, 2)], zrecv_sem.at[n])
        total = zpart[n, s] + zrecv[n, 0].astype(F32) + zrecv[n, 1].astype(F32)
        zfull[:, lanes(left + 1)] = total[:, 0:128]
        zfull[:, lanes(right + 1)] = total[:, 128:256]
        for e, t in ((0, 0), (1, row - 1)):
            if t in READY[n]:

                @pl.when(par > 0 if e == 0 else par < 3)
                def _(e=e):
                    drain(hrecv.at[e], hrecv_sem.at[e])

                edge = hrecv[e, 0].astype(F32)
                for o in range(1, 4):
                    edge = edge + hrecv[e, o].astype(F32)
                for j in range(8):
                    shift = 127 - j if e == 0 else (128 - j) % 128
                    moved = edge if shift == 0 else pltpu.roll(edge, shift, 1)
                    zfull[8 * j : 8 * j + 8, lanes(0 if e == 0 else row + 1)] = moved
        for t in READY[n]:
            before, here, after = (zfull[:, lanes(t + i)] for i in range(3))
            low = jnp.where(lane64 == 0, pltpu.roll(before, 1, 1), pltpu.roll(here, 1, 1))
            high = jnp.where(lane64 == 127, pltpu.roll(after, 127, 1), pltpu.roll(here, 127, 1))
            smooth = (0.5 * here + 0.25 * (low + high)) * scale_ref[:, lanes(t)]
            for q in range(2):
                halves = [smooth[32 * h + 16 * q : 32 * h + 16 * q + 16] for h in range(2)]
                wsend[t, q] = jnp.concatenate(halves, axis=0).astype(BF16)
        if n >= 2:
            upper = n - 2
            for mine in range(2):

                @pl.when(late == mine)
                def _(upper=upper, mine=mine):
                    for i, j in STEPS:
                        if (i + j + mine + upper) % 2 == 0:
                            to_y, to_x = (y + j) % 4, (x + i) % 4
                            t = 4 * upper + 2 * (to_y % 2) + to_x // 2
                            pltpu.make_async_remote_copy(
                                wsend.at[t, to_y // 2], wrecv.at[f], send_sem.at[4], recv_sem.at[4],
                                device_id={"freq": 4 * to_y + to_x}, device_id_type=MESH,
                            ).start()
                    if mine == upper:
                        own = wsend.at[4 * upper + 2 * (y % 2) + x // 2, y // 2]
                        pltpu.make_async_copy(own, wrecv.at[f], recv_sem.at[4]).start()

    drain(wrecv, recv_sem.at[4])
    spectra = wrecv[...].reshape(512, 128)
    for half in range(2):
        rows = slice(256 * half, 256 * half + 256)
        image = jnp.dot(table_hi[rows, :], spectra, preferred_element_type=F32)
        image = image + jnp.dot(table_lo[rows, :], spectra, preferred_element_type=F32)
        isend[8 * half : 8 * half + 8] = image.astype(BF16).reshape(8, 32, 128)
        for j in (0, 1) if half == 0 else (3, 2):
            row_y = (y + 2 + j) % 4
            for i in (2, 1, 3, 0):
                if i > 0 or j != 2:
                    target_x = (x + i) % 4
                    pltpu.make_async_remote_copy(
                        isend.at[4 * j + target_x], irecv.at[slot], send_sem.at[5], recv_sem.at[5 + late],
                        device_id={"freq": 4 * row_y + target_x}, device_id_type=MESH,
                    ).start()
    pltpu.make_async_copy(isend.at[8 + x], irecv.at[slot], recv_sem.at[5 + late]).start()

    for g in range(2):
        drain(arecv.at[g, pl.ds(0, 3)], send_sem.at[g])
        drain(brecv.at[g, pl.ds(0, 7)], send_sem.at[2 + g])
    for n in range(12):
        drain(zfwd.at[0, 0], zsend_sem.at[n])

    @pl.when(par > 0)
    def _():
        drain(hsend.at[0], hsend_sem.at[0])

    @pl.when(par < 3)
    def _():
        drain(hsend.at[1], hsend_sem.at[1])

    drain(wrecv.at[pl.ds(0, 15)], send_sem.at[4])
    drain(isend.at[pl.ds(0, 15)], send_sem.at[5])
    out_copies = []
    for last in range(2):
        drain(irecv.at[pl.ds(0, 8)], recv_sem.at[5 + last])
        for q in range(2):
            for t in range(4):
                piece = irecv[8 * q + 4 * last + t, 0:26, :].astype(F32)
                out_v[last, pl.ds(2 * t + q, 26, stride=8), :] = piece
        out_copies.append(
            pltpu.make_async_copy(
                out_v.at[last, pl.ds(0, 208)].reshape(26, 8, 128), out_ref.at[:, pl.ds(8 * last, 8)], local_sem.at[last]
            )
        )
        out_copies[-1].start()
    for copy in out_copies:
        copy.wait()


def local(series, kern, prior_spectrum, prior_scale):
    sensors, params = kern.shape[2:]
    series, kern = series.transpose(2, 0, 1), kern.transpose(0, 2, 1, 3)
    vmem = pltpu.VMEM
    dma = pltpu.SemaphoreType.DMA
    operands = (series, kern, prior_spectrum, prior_scale.reshape(1, -1))
    image = pl.pallas_call(
        kernel,
        out_shape=jax.ShapeDtypeStruct((26, 16, 128), F32),
        in_specs=[
            pl.BlockSpec(memory_space=pl.ANY),
        ] * 4,
        out_specs=pl.BlockSpec(memory_space=pl.ANY),
        scratch_shapes=[
            pltpu.SMEM((16,), F32),
            vmem((1, params), F32),
            vmem((26, 8, sensors), BF16),
            vmem((2, 2, sensors, 8, params), BF16),
            vmem((2, 256, 128), F32),
            vmem((2, 32, 384), F32),
            vmem((2, 4, 32, 384), BF16),
            vmem((2, 4, 32, 384), BF16),
            vmem((2, 8, 32, 384), BF16),
            vmem((2, 2, 64, 256), BF16),
            vmem((2, 2, 64, 256 * pl.cdiv(8 * sensors, 256)), BF16),
            vmem((2, 2, 64, 256 * pl.cdiv(8 * sensors, 256)), BF16),
            vmem((4, 4, 64, 256), BF16),
            vmem((4, 4, 64, 256), F32),
            vmem((4, 2, 64, 256), BF16),
            vmem((4, 4, 64, 256), BF16),
            vmem((64, 1280), F32),
            vmem((2, 4, 8, 128), BF16),
            vmem((2, 4, 8, 128), BF16),
            vmem((8, 2, 32, 128), BF16),
            vmem((16, 32, 128), BF16),
            vmem((16, 32, 128), BF16),
            vmem((16, 32, 128), BF16),
            vmem((2, 256, 128), F32),
            vmem((512, 512), BF16),
            vmem((512, 512), BF16),
            dma((7,)),
            dma((6,)),
            dma((7,)),
            dma((12,)),
            dma((13,)),
            dma((2,)),
            dma((2,)),
            pltpu.SemaphoreType.REGULAR((4,)),
        ],
        compiler_params=pltpu.CompilerParams(
            collective_id=0, has_side_effects=True, vmem_limit_bytes=50 * 1024 * 1024
        ),
        name="adjoint",
    )(*(pltpu.with_memory_space_constraint(v, pltpu.HBM) for v in operands))
    return image.reshape(26, 8, 2, 128).transpose(0, 2, 1, 3).reshape(26, 2, params)


def solution(mesh):
    placed = (P(None, "sens", "freq"), P(None, "freq", "sens", "param"), P("freq"), P("param"))
    return jax.shard_map(
        local, mesh=mesh, in_specs=placed, out_specs=P("freq", "sens", "param"), check_vma=False
    )
```

```python
import functools
import math

import jax
import jax.numpy as jnp
from jax import lax
from jax.experimental import pallas as pl
from jax.experimental.pallas import tpu as pltpu
from jax.sharding import PartitionSpec as P

LEN = 840
MESH = pl.DeviceIdType.MESH
F32, BF16 = jnp.float32, jnp.bfloat16
CHUNKS = ((0, 7), (1, 2), (3, 4), (5, 6))
READY = ((), (), (0, 1, 2, 3), (4, 5, 6, 7))
STEPS = sorted(((i, j) for i in range(4) for j in range(4) if i + j), key=lambda v: -sum(min(a, 4 - a) for a in v))


def iota(shape, dim):
    return lax.broadcasted_iota(jnp.int32, shape, dim)


def turned_cos(bins, times, part):
    turn = bins.astype(F32) * times.astype(F32) + (LEN // 4) * part.astype(F32)
    turn = turn - LEN * jnp.floor(turn * (1.0 / LEN) + 0.5)
    half = turn * (math.pi / LEN)
    square = half * half
    term = 1.0 / 6227020800.0
    for coef in (-1.0 / 39916800.0, 1.0 / 362880.0, -1.0 / 5040.0, 1.0 / 120.0, -1.0 / 6.0, 1.0):
        term = term * square + coef
    sine = half * term
    return 1.0 - 2.0 * sine * sine


def split(x):
    high = x.astype(BF16)
    return high, (x - high.astype(F32)).astype(BF16)


def kernel(
    series_ref, kern_ref, prior_hbm, scale_hbm, out_ref,
    prior_ref, scale_ref, ser_v, kern_v, by_time, turned, arecv, bsend, brecv, packed, lhs_re, lhs_im, zsend, zpart, zfwd, zrecv, zfull,
    hsend, hrecv, wsend, wrecv, isend, irecv, out_v, spreads, table_hi, table_lo,
    local_sem, send_sem, recv_sem, zsend_sem, zrecv_sem, hsend_sem, hrecv_sem, round_sem,
):
    f, par, s = lax.axis_index("freq"), lax.axis_index("param"), lax.axis_index("sens")
    y, x = f // 4, f % 4
    core = par % 2
    sensors = ser_v.shape[2]
    row = kern_v.shape[4] // 128
    rest_of = sensors - 128
    late = 1 - (x + y) % 2
    slot = 8 * (y // 2) + 2 * (y % 2) + x // 2 + 4 * late
    end = (s == 0) | (s == 3)
    middle = (s == 1) | (s == 2)
    near, beyond = 1 + s // 3, 2 - s // 3
    across = 3 - s
    side = jnp.where(end, near, 3 * (s - 1))
    far = jnp.where(end, across, 6 - 3 * s)
    first_at = lambda j: j * (1 + 3 * core) + 4 * y * (1 - core) + x * core
    second_at = lambda m: m * (4 - 3 * core) + x * (1 - core) + 4 * y * core
    first_pos = x * (1 - core) + y * core
    second_pos = y * (1 - core) + x * core

    series_in = pltpu.make_async_copy(series_ref, ser_v, local_sem.at[0])
    series_in.start()
    barrier = pltpu.get_barrier_semaphore()
    other = par + 1 - 2 * core
    in_plane = [{"freq": first_at((first_pos + o) % 4)} for o in (2, 1, 3)] + [{"param": other}]

    def greet(sem, peers):
        for peer in peers:
            pl.semaphore_signal(sem, 1, device_id=peer, device_id_type=MESH)

    greet(barrier, in_plane)
    for o in range(1, 4):

        @pl.when(s + o < 4)
        def _(o=o):
            greet(barrier, [{"sens": s + o}, {"sens": s + o, "param": other}])

    @pl.when(par == 1)
    def _():
        greet(barrier, [{"sens": d, "param": 2} for d in range(4)])

    small_in = []
    for n, (source, target) in enumerate(((prior_hbm, prior_ref), (scale_hbm, scale_ref))):
        small_in.append(pltpu.make_async_copy(source, target, local_sem.at[5 + n]))
        small_in[-1].start()
    kernel_in = []
    for p in range(2):
        for h in range(2):
            kernel_in.append(
                pltpu.make_async_copy(
                    kern_ref.at[p, :, pl.ds(8 * h, 8)], kern_v.at[h, p], local_sem.at[1 + 2 * h + p]
                )
            )
            kernel_in[-1].start()

    ri, ci = iota((128, 128), 0), iota((128, 128), 1)
    bins = 16 * second_at(ri >> 5) + (ri & 15)
    inside = ci & 31
    times = 26 * first_at(ci >> 5) + inside
    forward = jnp.where(inside < 26, turned_cos(bins, times, (ri >> 4) & 1), 0.0)
    fwd_hi, fwd_lo = split(forward)

    turned[:, 24:32, :] = jnp.zeros((2, 8, 384), F32)
    turned[:, :, 256:384] = jnp.zeros((2, 32, 128), F32)
    series_in.wait()
    by_time[0, 0:208, :] = ser_v[:, :, 0:128].astype(F32).reshape(208, 128)
    by_time[1, 0:208, 0:rest_of] = ser_v[:, :, 128:sensors].astype(F32).reshape(208, rest_of)
    for g in range(2):
        for q in range(2):
            rows = pl.ds((6 * core if g == 0 else 2 + 2 * core) + q, 26, stride=8)
            turned[g, 0:26, 128 * q : 128 * q + 128] = by_time[0, rows, :]
            turned[g, 0:26, 256 + 32 * q : 256 + 32 * q + rest_of] = by_time[1, rows, :][:, 0:rest_of]
        arecv[g, first_pos] = turned[g].astype(BF16)

    pl.semaphore_wait(barrier, 4 + 2 * s + jnp.where(par == 2, 4, 0))

    for g in range(2):
        for o in (2, 1, 3):
            pltpu.make_async_remote_copy(
                arecv.at[g, first_pos], arecv.at[g, first_pos], send_sem.at[g], recv_sem.at[g],
                device_id={"freq": first_at((first_pos + o) % 4)}, device_id_type=MESH,
            ).start()

    greet(round_sem.at[0], in_plane)

    for o in range(1, 4):

        @pl.when(s >= o)
        def _(o=o):
            greet(round_sem.at[2], [{"sens": s - o}])
            greet(round_sem.at[3], [{"sens": s - o, "param": other}])

    @pl.when(par == 2)
    def _():
        greet(round_sem.at[3], [{"sens": d, "param": 1} for d in range(4)])

    @pl.loop(0, 16)
    def _(b):
        ti, ki = iota((32, 512), 0), iota((32, 512), 1)
        owner = 4 * ((y + 2 + b // 4) % 4) + b % 4
        values = turned_cos(((ki >> 5) << 4) + ((ki >> 4) & 1) * 8 + (ki & 7), 26 * owner + ti, (ki >> 3) & 1)
        high, low = split(values)
        rows = pl.ds(pl.multiple_of(32 * b, 32), 32)
        table_hi[rows, :] = high
        table_lo[rows, :] = low

    def drain(like, sem):
        pltpu.make_async_copy(like, like, sem).wait()

    for at in range(0, 8 * sensors, 256):
        size = min(256, 8 * sensors - at)
        spread = (iota((sensors, size), 0) == (at + iota((sensors, size), 1)) // 8).astype(BF16)
        spreads[0:sensors, at : at + size] = spread

    pl.semaphore_wait(round_sem.at[0], 4)
    greet(round_sem.at[1], in_plane)
    for g in range(2):
        drain(arecv.at[g, pl.ds(0, 3)], recv_sem.at[g])
        gathered = arecv[g].reshape(128, 384)
        spec = jnp.dot(fwd_hi, gathered, preferred_element_type=F32)
        spec = spec + jnp.dot(fwd_lo, gathered, preferred_element_type=F32)
        spec = spec * (1.0 / math.sqrt(416.0))
        bsend[g] = spec.astype(BF16).reshape(4, 32, 384)
        if g == 0:
            pl.semaphore_wait(round_sem.at[1], 4)
        for o in (2, 1, 3, 0):
            m = (second_pos + o) % 4
            for c in range(2):
                if o + c > 0:
                    target = par + (1 - 2 * core) * c
                    pltpu.make_async_remote_copy(
                        bsend.at[g, m], brecv.at[g, 4 * core + second_pos],
                        send_sem.at[2 + g], recv_sem.at[2 + g],
                        device_id={"freq": second_at(m), "param": target}, device_id_type=MESH,
                    ).start()
        brecv[g, 4 * core + second_pos] = bsend[g, second_pos]

    lane = iota((32, 128), 1)
    width = 8 * sensors
    diagonal = iota((16, 256), 0) % 8 == iota((16, 256), 1) % 8

    def spread_out(g):
        for c in range(2):
            total = brecv[g, 4 * c].astype(F32)
            for m in range(1, 4):
                total = total + brecv[g, 4 * c + m].astype(F32)
            for q in range(2):
                tail = total[:, 256:384]
                tail = tail if q == 0 else pltpu.roll(tail, 128 - 32 * q, 1)
                tail = jnp.where(lane < 32, tail, 0.0)
                wide = jnp.concatenate([total[:, 128 * q : 128 * q + 128], tail], axis=1)
                for h in range(2):
                    pair = [wide[16 * p + 8 * h : 16 * p + 8 * h + 8] for p in range(2)]
                    packed[g, h, pl.ds(32 * c + 16 * q, 16), :] = jnp.concatenate(pair, axis=0).astype(BF16)
        compact = packed[g].reshape(128, 256)[:, 0:sensors]
        for at in range(0, width, 256):
            size = min(256, width - at)
            spaced = jnp.dot(compact, spreads[0:sensors, at : at + size], preferred_element_type=F32)
            for r in range(8):
                block = jnp.where(diagonal[:, 0:size], spaced[16 * r : 16 * r + 16], 0.0)
                rows = slice(16 * (r % 4), 16 * (r % 4) + 16)
                lhs_re[g, r // 4, rows, at : at + size] = block.astype(BF16)
                swapped = jnp.concatenate([block[8:16], -block[0:8]], axis=0)
                lhs_im[g, r // 4, rows, at : at + size] = swapped.astype(BF16)

    drain(brecv.at[0, pl.ds(0, 7)], recv_sem.at[2])
    spread_out(0)
    for copy in small_in + kernel_in:
        copy.wait()

    @pl.when(s < 3)
    def _():
        pl.semaphore_wait(round_sem.at[2], 3 - s)


    def send_along(source, target, kind, n, received, to):
        pltpu.make_async_remote_copy(
            source, target, zsend_sem.at[4 * kind + n], zrecv_sem.at[received],
            device_id={"sens": to}, device_id_type=MESH,
        ).start()

    def lanes(tile, count=1):
        return slice(128 * tile, 128 * (tile + count))

    eighth = iota((8, 256), 0)
    weights = []
    for h in range(2):
        column = jnp.zeros((8, 256), F32)
        for k in range(8):
            column = jnp.where(eighth == k, prior_ref[8 * h + k] * (1.0 / 16.0), column)
        weights.append(column)

    def lead(n):
        source, to = jnp.where(end, across, side), jnp.where(end, near, side)
        kind = jnp.where(end, 1, 0)
        send_along(zsend.at[n, source], zrecv.at[n, 2 * kind], 0, n, 4 * kind + n, to)

    def contract(g, n):
        left, right = CHUNKS[n]
        scale = jnp.concatenate([scale_ref[:, lanes(left)], scale_ref[:, lanes(right)]], axis=1)
        for h in range(2):
            product = jnp.zeros((64, 256), F32)
            for p, lhs in ((0, lhs_re), (1, lhs_im)):
                operand = jnp.concatenate(
                    [kern_v[h, p, :, :, lanes(left)], kern_v[h, p, :, :, lanes(right)]], axis=2
                ).reshape(width, 256)
                product = product + jnp.dot(lhs[g, h, :, 0:width], operand, preferred_element_type=F32)
            factor = jnp.concatenate([weights[h] * scale] * 4, axis=0)
            for c, d in enumerate((1, 2) if g else (0, 3)):
                piece = product[32 * c : 32 * c + 32] * factor
                zpart[n, d, pl.ds(32 * h, 32), :] = piece
                zsend[n, d, pl.ds(32 * h, 32), :] = piece.astype(BF16)

    def parts_of(kind, n):
        return [pl.ds(16 * m, 16) for m in range(4)] if kind == 1 and n == 3 else [pl.ds(0, 64)]

    def pass_on(kind, n):
        @pl.when(middle)
        def _():
            to = across if kind else far
            for m, part in enumerate(parts_of(kind, n)):
                drain(zrecv.at[n, 2 + kind, part], zrecv_sem.at[11 + m if m else 4 + 4 * kind + n])
                both = zpart[n, to, part] + zrecv[n, 2 + kind, part].astype(F32)
                zfwd[n, kind, part] = both.astype(BF16)
                send_along(zfwd.at[n, kind, part], zrecv.at[n, 1, part], 1 + kind, n, n, to)

    lane8 = iota((8, 128), 1)

    @pl.when(par == 0)
    def _():
        hrecv[0] = jnp.zeros((4, 8, 128), BF16)

    @pl.when(par == 3)
    def _():
        hrecv[1] = jnp.zeros((4, 8, 128), BF16)

    def send_edges(g):
        for d in (1, 2) if g else (0, 3):
            for e in range(2):
                columns = jnp.zeros((8, 128), F32)
                for j in range(8):
                    block = zpart[0, d, 8 * j : 8 * j + 8, lanes(e)]
                    moved = block if j + e == 0 else pltpu.roll(block, j + e, 1)
                    columns = jnp.where(lane8 == j, moved, columns)
                hsend[e, d] = columns.astype(BF16)

        @pl.when(par > 0)
        def _():
            for d in (1, 2) if g else (0, 3):
                pltpu.make_async_remote_copy(
                    hsend.at[0, d], hrecv.at[1, s], hsend_sem.at[0], hrecv_sem.at[1],
                    device_id={"param": par - 1, "sens": d}, device_id_type=MESH,
                ).start()

        @pl.when(par < 3)
        def _():
            for d in (1, 2) if g else (0, 3):
                pltpu.make_async_remote_copy(
                    hsend.at[1, d], hrecv.at[0, s], hsend_sem.at[1], hrecv_sem.at[0],
                    device_id={"param": par + 1, "sens": d}, device_id_type=MESH,
                ).start()

    for n in range(4):
        contract(0, n)
        lead(n)
    drain(brecv.at[1, pl.ds(0, 7)], recv_sem.at[3])
    spread_out(1)
    for n in range(4):
        contract(1, n)

        @pl.when(end)
        def _(n=n):
            for m, part in enumerate(parts_of(1, n)):
                send_along(zsend.at[n, beyond, part], zrecv.at[n, 3, part], 1, n, 11 + m if m else 8 + n, near)

        if n == 0:

            @pl.when((s < 3) | (par == 1))
            def _():
                pl.semaphore_wait(round_sem.at[3], 3 - s + jnp.where(par == 1, 4, 0))

            send_edges(0)
            send_edges(1)
        if n == 1:
            pass_on(0, 0)
        if n == 2:
            pass_on(0, 1)

    def give_rest():
        for n in range(4):
            send_along(zsend.at[n, near], zrecv.at[n, 0], 2, n, n, near)

    pl.when(end)(give_rest)
    for kind, n in ((0, 2), (0, 3), (1, 0), (1, 1), (1, 2), (1, 3)):
        pass_on(kind, n)

    lane64 = iota((64, 128), 1)
    for n, (left, right) in enumerate(CHUNKS):
        drain(zrecv.at[n, pl.ds(0, 2)], zrecv_sem.at[n])
        total = zpart[n, s] + zrecv[n, 0].astype(F32) + zrecv[n, 1].astype(F32)
        zfull[:, lanes(left + 1)] = total[:, 0:128]
        zfull[:, lanes(right + 1)] = total[:, 128:256]
        for e, t in ((0, 0), (1, row - 1)):
            if t in READY[n]:

                @pl.when(par > 0 if e == 0 else par < 3)
                def _(e=e):
                    drain(hrecv.at[e], hrecv_sem.at[e])

                edge = hrecv[e, 0].astype(F32)
                for o in range(1, 4):
                    edge = edge + hrecv[e, o].astype(F32)
                for j in range(8):
                    shift = 127 - j if e == 0 else (128 - j) % 128
                    moved = edge if shift == 0 else pltpu.roll(edge, shift, 1)
                    zfull[8 * j : 8 * j + 8, lanes(0 if e == 0 else row + 1)] = moved
        for t in READY[n]:
            before, here, after = (zfull[:, lanes(t + i)] for i in range(3))
            low = jnp.where(lane64 == 0, pltpu.roll(before, 1, 1), pltpu.roll(here, 1, 1))
            high = jnp.where(lane64 == 127, pltpu.roll(after, 127, 1), pltpu.roll(here, 127, 1))
            smooth = (0.5 * here + 0.25 * (low + high)) * scale_ref[:, lanes(t)]
            for q in range(2):
                halves = [smooth[32 * h + 16 * q : 32 * h + 16 * q + 16] for h in range(2)]
                wsend[t, q] = jnp.concatenate(halves, axis=0).astype(BF16)
        if n >= 2:
            upper = n - 2
            for mine in range(2):

                @pl.when(late == mine)
                def _(upper=upper, mine=mine):
                    for i, j in STEPS:
                        if (i + j + mine + upper) % 2 == 0:
                            to_y, to_x = (y + j) % 4, (x + i) % 4
                            t = 4 * upper + 2 * (to_y % 2) + to_x // 2
                            pltpu.make_async_remote_copy(
                                wsend.at[t, to_y // 2], wrecv.at[f], send_sem.at[4], recv_sem.at[4],
                                device_id={"freq": 4 * to_y + to_x}, device_id_type=MESH,
                            ).start()
                    if mine == upper:
                        own = wsend.at[4 * upper + 2 * (y % 2) + x // 2, y // 2]
                        pltpu.make_async_copy(own, wrecv.at[f], recv_sem.at[4]).start()

    drain(wrecv, recv_sem.at[4])
    spectra = wrecv[...].reshape(512, 128)
    for half in range(2):
        rows = slice(256 * half, 256 * half + 256)
        image = jnp.dot(table_hi[rows, :], spectra, preferred_element_type=F32)
        image = image + jnp.dot(table_lo[rows, :], spectra, preferred_element_type=F32)
        isend[8 * half : 8 * half + 8] = image.astype(BF16).reshape(8, 32, 128)
        for j in (0, 1) if half == 0 else (3, 2):
            row_y = (y + 2 + j) % 4
            for i in (2, 1, 3, 0):
                if i > 0 or j != 2:
                    target_x = (x + i) % 4
                    pltpu.make_async_remote_copy(
                        isend.at[4 * j + target_x], irecv.at[slot], send_sem.at[5], recv_sem.at[5 + late],
                        device_id={"freq": 4 * row_y + target_x}, device_id_type=MESH,
                    ).start()
    pltpu.make_async_copy(isend.at[8 + x], irecv.at[slot], recv_sem.at[5 + late]).start()

    for g in range(2):
        drain(arecv.at[g, pl.ds(0, 3)], send_sem.at[g])
        drain(brecv.at[g, pl.ds(0, 7)], send_sem.at[2 + g])
    for n in range(12):
        drain(zfwd.at[0, 0], zsend_sem.at[n])

    @pl.when(par > 0)
    def _():
        drain(hsend.at[0], hsend_sem.at[0])

    @pl.when(par < 3)
    def _():
        drain(hsend.at[1], hsend_sem.at[1])

    drain(wrecv.at[pl.ds(0, 15)], send_sem.at[4])
    drain(isend.at[pl.ds(0, 15)], send_sem.at[5])
    out_copies = []
    for last in range(2):
        drain(irecv.at[pl.ds(0, 8)], recv_sem.at[5 + last])
        for q in range(2):
            for t in range(4):
                piece = irecv[8 * q + 4 * last + t, 0:26, :].astype(F32)
                out_v[last, pl.ds(2 * t + q, 26, stride=8), :] = piece
        out_copies.append(
            pltpu.make_async_copy(
                out_v.at[last, pl.ds(0, 208)].reshape(26, 8, 128), out_ref.at[:, pl.ds(8 * last, 8)], local_sem.at[last]
            )
        )
        out_copies[-1].start()
    for copy in out_copies:
        copy.wait()


def local(series, kern, prior_spectrum, prior_scale):
    sensors, params = kern.shape[2:]
    series, kern = series.transpose(2, 0, 1), kern.transpose(0, 2, 1, 3)
    vmem = pltpu.VMEM
    dma = pltpu.SemaphoreType.DMA
    operands = (series, kern, prior_spectrum, prior_scale.reshape(1, -1))
    image = pl.pallas_call(
        kernel,
        out_shape=jax.ShapeDtypeStruct((26, 16, 128), F32),
        in_specs=[
            pl.BlockSpec(memory_space=pl.ANY),
        ] * 4,
        out_specs=pl.BlockSpec(memory_space=pl.ANY),
        scratch_shapes=[
            pltpu.SMEM((16,), F32),
            vmem((1, params), F32),
            vmem((26, 8, sensors), BF16),
            vmem((2, 2, sensors, 8, params), BF16),
            vmem((2, 256, 128), F32),
            vmem((2, 32, 384), F32),
            vmem((2, 4, 32, 384), BF16),
            vmem((2, 4, 32, 384), BF16),
            vmem((2, 8, 32, 384), BF16),
            vmem((2, 2, 64, 256), BF16),
            vmem((2, 2, 64, 256 * pl.cdiv(8 * sensors, 256)), BF16),
            vmem((2, 2, 64, 256 * pl.cdiv(8 * sensors, 256)), BF16),
            vmem((4, 4, 64, 256), BF16),
            vmem((4, 4, 64, 256), F32),
            vmem((4, 2, 64, 256), BF16),
            vmem((4, 4, 64, 256), BF16),
            vmem((64, 1280), F32),
            vmem((2, 4, 8, 128), BF16),
            vmem((2, 4, 8, 128), BF16),
            vmem((8, 2, 32, 128), BF16),
            vmem((16, 32, 128), BF16),
            vmem((16, 32, 128), BF16),
            vmem((16, 32, 128), BF16),
            vmem((2, 256, 128), F32),
            vmem((pl.cdiv(sensors, 16) * 16, 256 * pl.cdiv(8 * sensors, 256)), BF16),
            vmem((512, 512), BF16),
            vmem((512, 512), BF16),
            dma((7,)),
            dma((6,)),
            dma((7,)),
            dma((12,)),
            dma((15,)),
            dma((2,)),
            dma((2,)),
            pltpu.SemaphoreType.REGULAR((4,)),
        ],
        compiler_params=pltpu.CompilerParams(
            collective_id=0, has_side_effects=True, vmem_limit_bytes=50 * 1024 * 1024
        ),
        name="adjoint",
    )(*(pltpu.with_memory_space_constraint(v, pltpu.HBM) for v in operands))
    return image.reshape(26, 8, 2, 128).transpose(0, 2, 1, 3).reshape(26, 2, params)


def solution(mesh):
    placed = (P(None, "sens", "freq"), P(None, "freq", "sens", "param"), P("freq"), P("param"))
    return jax.shard_map(
        local, mesh=mesh, in_specs=placed, out_specs=P("freq", "sens", "param"), check_vma=False
    )
```

```python
import functools
import math

import jax
import jax.numpy as jnp
from jax import lax
from jax.experimental import pallas as pl
from jax.experimental.pallas import tpu as pltpu
from jax.sharding import PartitionSpec as P

LEN = 840
MESH = pl.DeviceIdType.MESH
F32, BF16 = jnp.float32, jnp.bfloat16
CHUNKS = ((0, 7), (1, 2), (3, 4), (5, 6))
READY = ((), (), (0, 1, 2, 3), (4, 5, 6, 7))
STEPS = sorted(((i, j) for i in range(4) for j in range(4) if i + j), key=lambda v: -sum(min(a, 4 - a) for a in v))


def iota(shape, dim):
    return lax.broadcasted_iota(jnp.int32, shape, dim)


def turned_cos(bins, times, part):
    turn = bins.astype(F32) * times.astype(F32) + (LEN // 4) * part.astype(F32)
    turn = turn - LEN * jnp.floor(turn * (1.0 / LEN) + 0.5)
    half = turn * (math.pi / LEN)
    square = half * half
    term = 1.0 / 6227020800.0
    for coef in (-1.0 / 39916800.0, 1.0 / 362880.0, -1.0 / 5040.0, 1.0 / 120.0, -1.0 / 6.0, 1.0):
        term = term * square + coef
    sine = half * term
    return 1.0 - 2.0 * sine * sine


def split(x):
    high = x.astype(BF16)
    return high, (x - high.astype(F32)).astype(BF16)


def kernel(
    series_ref, kern_ref, prior_hbm, scale_hbm, out_ref,
    prior_ref, scale_ref, ser_v, kern_v, by_time, turned, arecv, bsend, brecv, packed, lhs_re, lhs_im, zsend, zpart, zfwd, zrecv, zfull,
    hsend, hrecv, wsend, wrecv, isend, irecv, out_v, table_hi, table_lo,
    local_sem, send_sem, recv_sem, zsend_sem, zrecv_sem, hsend_sem, hrecv_sem, round_sem,
):
    f, par, s = lax.axis_index("freq"), lax.axis_index("param"), lax.axis_index("sens")
    y, x = f // 4, f % 4
    core = par % 2
    sensors = ser_v.shape[2]
    row = kern_v.shape[4] // 128
    rest_of = sensors - 128
    late = 1 - (x + y) % 2
    slot = 8 * (y // 2) + 2 * (y % 2) + x // 2 + 4 * late
    end = (s == 0) | (s == 3)
    middle = (s == 1) | (s == 2)
    near, beyond = 1 + s // 3, 2 - s // 3
    across = 3 - s
    side = jnp.where(end, near, 3 * (s - 1))
    far = jnp.where(end, across, 6 - 3 * s)
    first_at = lambda j: j * (1 + 3 * core) + 4 * y * (1 - core) + x * core
    second_at = lambda m: m * (4 - 3 * core) + x * (1 - core) + 4 * y * core
    first_pos = x * (1 - core) + y * core
    second_pos = y * (1 - core) + x * core

    barrier = pltpu.get_barrier_semaphore()
    other = par + 1 - 2 * core
    in_plane = [{"freq": first_at((first_pos + o) % 4)} for o in (2, 1, 3)] + [{"param": other}]

    def greet(sem, peers):
        for peer in peers:
            pl.semaphore_signal(sem, 1, device_id=peer, device_id_type=MESH)

    greet(barrier, in_plane)
    series_in = pltpu.make_async_copy(series_ref, ser_v, local_sem.at[0])
    series_in.start()
    for o in range(1, 4):

        @pl.when(s + o < 4)
        def _(o=o):
            greet(barrier, [{"sens": s + o}, {"sens": s + o, "param": other}])

    @pl.when(par == 1)
    def _():
        greet(barrier, [{"sens": d, "param": 2} for d in range(4)])

    small_in = []
    for n, (source, target) in enumerate(((prior_hbm, prior_ref), (scale_hbm, scale_ref))):
        small_in.append(pltpu.make_async_copy(source, target, local_sem.at[5 + n]))
        small_in[-1].start()
    kernel_in = []
    for p in range(2):
        for h in range(2):
            kernel_in.append(
                pltpu.make_async_copy(
                    kern_ref.at[p, :, pl.ds(8 * h, 8)], kern_v.at[h, p], local_sem.at[1 + 2 * h + p]
                )
            )

    ri, ci = iota((128, 128), 0), iota((128, 128), 1)
    bins = 16 * second_at(ri >> 5) + (ri & 15)
    inside = ci & 31
    times = 26 * first_at(ci >> 5) + inside
    forward = jnp.where(inside < 26, turned_cos(bins, times, (ri >> 4) & 1), 0.0)
    fwd_hi, fwd_lo = split(forward)

    turned[:, 24:32, :] = jnp.zeros((2, 8, 384), F32)
    turned[:, :, 256:384] = jnp.zeros((2, 32, 128), F32)
    series_in.wait()
    for copy in kernel_in:
        copy.start()
    by_time[0, 0:208, :] = ser_v[:, :, 0:128].astype(F32).reshape(208, 128)
    by_time[1, 0:208, 0:rest_of] = ser_v[:, :, 128:sensors].astype(F32).reshape(208, rest_of)
    for g in range(2):
        for q in range(2):
            rows = pl.ds((6 * core if g == 0 else 2 + 2 * core) + q, 26, stride=8)
            turned[g, 0:26, 128 * q : 128 * q + 128] = by_time[0, rows, :]
            turned[g, 0:26, 256 + 32 * q : 256 + 32 * q + rest_of] = by_time[1, rows, :][:, 0:rest_of]
        arecv[g, first_pos] = turned[g].astype(BF16)

    pl.semaphore_wait(barrier, 4 + 2 * s + jnp.where(par == 2, 4, 0))

    for g in range(2):
        for o in (2, 1, 3):
            pltpu.make_async_remote_copy(
                arecv.at[g, first_pos], arecv.at[g, first_pos], send_sem.at[g], recv_sem.at[g],
                device_id={"freq": first_at((first_pos + o) % 4)}, device_id_type=MESH,
            ).start()

    greet(round_sem.at[0], in_plane)

    for o in range(1, 4):

        @pl.when(s >= o)
        def _(o=o):
            greet(round_sem.at[2], [{"sens": s - o}])
            greet(round_sem.at[3], [{"sens": s - o, "param": other}])

    @pl.when(par == 2)
    def _():
        greet(round_sem.at[3], [{"sens": d, "param": 1} for d in range(4)])

    @pl.loop(0, 16)
    def _(b):
        ti, ki = iota((32, 512), 0), iota((32, 512), 1)
        owner = 4 * ((y + 2 + b // 4) % 4) + b % 4
        values = turned_cos(((ki >> 5) << 4) + ((ki >> 4) & 1) * 8 + (ki & 7), 26 * owner + ti, (ki >> 3) & 1)
        high, low = split(values)
        rows = pl.ds(pl.multiple_of(32 * b, 32), 32)
        table_hi[rows, :] = high
        table_lo[rows, :] = low

    def drain(like, sem):
        pltpu.make_async_copy(like, like, sem).wait()

    pl.semaphore_wait(round_sem.at[0], 4)
    greet(round_sem.at[1], in_plane)
    for g in range(2):
        drain(arecv.at[g, pl.ds(0, 3)], recv_sem.at[g])
        gathered = arecv[g].reshape(128, 384)
        spec = jnp.dot(fwd_hi, gathered, preferred_element_type=F32)
        spec = spec + jnp.dot(fwd_lo, gathered, preferred_element_type=F32)
        spec = spec * (1.0 / math.sqrt(416.0))
        bsend[g] = spec.astype(BF16).reshape(4, 32, 384)
        if g == 0:
            pl.semaphore_wait(round_sem.at[1], 4)
        for o in (2, 1, 3, 0):
            m = (second_pos + o) % 4
            for c in range(2):
                if o + c > 0:
                    target = par + (1 - 2 * core) * c
                    pltpu.make_async_remote_copy(
                        bsend.at[g, m], brecv.at[g, 4 * core + second_pos],
                        send_sem.at[2 + g], recv_sem.at[2 + g],
                        device_id={"freq": second_at(m), "param": target}, device_id_type=MESH,
                    ).start()
        brecv[g, 4 * core + second_pos] = bsend[g, second_pos]

    lane = iota((32, 128), 1)
    width = 8 * sensors
    diagonal = iota((16, 256), 0) % 8 == iota((16, 256), 1) % 8

    def spread_out(g):
        for c in range(2):
            total = brecv[g, 4 * c].astype(F32)
            for m in range(1, 4):
                total = total + brecv[g, 4 * c + m].astype(F32)
            for q in range(2):
                tail = total[:, 256:384]
                tail = tail if q == 0 else pltpu.roll(tail, 128 - 32 * q, 1)
                tail = jnp.where(lane < 32, tail, 0.0)
                wide = jnp.concatenate([total[:, 128 * q : 128 * q + 128], tail], axis=1)
                for h in range(2):
                    pair = [wide[16 * p + 8 * h : 16 * p + 8 * h + 8] for p in range(2)]
                    packed[g, h, pl.ds(32 * c + 16 * q, 16), :] = jnp.concatenate(pair, axis=0).astype(BF16)
        compact = packed[g].reshape(128, 256)[:, 0:sensors]
        for at in range(0, width, 256):
            size = min(256, width - at)
            spread = (iota((sensors, size), 0) == (at + iota((sensors, size), 1)) // 8).astype(BF16)
            spaced = jnp.dot(compact, spread, preferred_element_type=F32)
            for r in range(8):
                block = jnp.where(diagonal[:, 0:size], spaced[16 * r : 16 * r + 16], 0.0)
                rows = slice(16 * (r % 4), 16 * (r % 4) + 16)
                lhs_re[g, r // 4, rows, at : at + size] = block.astype(BF16)
                swapped = jnp.concatenate([block[8:16], -block[0:8]], axis=0)
                lhs_im[g, r // 4, rows, at : at + size] = swapped.astype(BF16)

    drain(brecv.at[0, pl.ds(0, 7)], recv_sem.at[2])
    spread_out(0)
    for copy in small_in + kernel_in:
        copy.wait()

    @pl.when(s < 3)
    def _():
        pl.semaphore_wait(round_sem.at[2], 3 - s)


    def send_along(source, target, kind, n, received, to):
        pltpu.make_async_remote_copy(
            source, target, zsend_sem.at[4 * kind + n], zrecv_sem.at[received],
            device_id={"sens": to}, device_id_type=MESH,
        ).start()

    def lanes(tile, count=1):
        return slice(128 * tile, 128 * (tile + count))

    eighth = iota((8, 256), 0)
    weights = []
    for h in range(2):
        column = jnp.zeros((8, 256), F32)
        for k in range(8):
            column = jnp.where(eighth == k, prior_ref[8 * h + k] * (1.0 / 16.0), column)
        weights.append(column)

    def lead(n):
        source, to = jnp.where(end, across, side), jnp.where(end, near, side)
        kind = jnp.where(end, 1, 0)
        send_along(zsend.at[n, source], zrecv.at[n, 2 * kind], 0, n, 4 * kind + n, to)

    def contract(g, n):
        left, right = CHUNKS[n]
        scale = jnp.concatenate([scale_ref[:, lanes(left)], scale_ref[:, lanes(right)]], axis=1)
        for h in range(2):
            product = jnp.zeros((64, 256), F32)
            for p, lhs in ((0, lhs_re), (1, lhs_im)):
                operand = jnp.concatenate(
                    [kern_v[h, p, :, :, lanes(left)], kern_v[h, p, :, :, lanes(right)]], axis=2
                ).reshape(width, 256)
                product = product + jnp.dot(lhs[g, h, :, 0:width], operand, preferred_element_type=F32)
            factor = jnp.concatenate([weights[h] * scale] * 4, axis=0)
            for c, d in enumerate((1, 2) if g else (0, 3)):
                piece = product[32 * c : 32 * c + 32] * factor
                zpart[n, d, pl.ds(32 * h, 32), :] = piece
                zsend[n, d, pl.ds(32 * h, 32), :] = piece.astype(BF16)

    def parts_of(kind, n):
        return (pl.ds(0, 32), pl.ds(32, 32)) if kind == 1 and n == 3 else (pl.ds(0, 64),)

    def pass_on(kind, n):
        @pl.when(middle)
        def _():
            to = across if kind else far
            for m, part in enumerate(parts_of(kind, n)):
                drain(zrecv.at[n, 2 + kind, part], zrecv_sem.at[12 if m else 4 + 4 * kind + n])
                both = zpart[n, to, part] + zrecv[n, 2 + kind, part].astype(F32)
                zfwd[n, kind, part] = both.astype(BF16)
                send_along(zfwd.at[n, kind, part], zrecv.at[n, 1, part], 1 + kind, n, n, to)

    lane8 = iota((8, 128), 1)

    @pl.when(par == 0)
    def _():
        hrecv[0] = jnp.zeros((4, 8, 128), BF16)

    @pl.when(par == 3)
    def _():
        hrecv[1] = jnp.zeros((4, 8, 128), BF16)

    def send_edges(g):
        for d in (1, 2) if g else (0, 3):
            for e in range(2):
                columns = jnp.zeros((8, 128), F32)
                for j in range(8):
                    block = zpart[0, d, 8 * j : 8 * j + 8, lanes(e)]
                    moved = block if j + e == 0 else pltpu.roll(block, j + e, 1)
                    columns = jnp.where(lane8 == j, moved, columns)
                hsend[e, d] = columns.astype(BF16)

        @pl.when(par > 0)
        def _():
            for d in (1, 2) if g else (0, 3):
                pltpu.make_async_remote_copy(
                    hsend.at[0, d], hrecv.at[1, s], hsend_sem.at[0], hrecv_sem.at[1],
                    device_id={"param": par - 1, "sens": d}, device_id_type=MESH,
                ).start()

        @pl.when(par < 3)
        def _():
            for d in (1, 2) if g else (0, 3):
                pltpu.make_async_remote_copy(
                    hsend.at[1, d], hrecv.at[0, s], hsend_sem.at[1], hrecv_sem.at[0],
                    device_id={"param": par + 1, "sens": d}, device_id_type=MESH,
                ).start()

    for n in range(4):
        contract(0, n)
        lead(n)
    drain(brecv.at[1, pl.ds(0, 7)], recv_sem.at[3])
    spread_out(1)
    for n in range(4):
        contract(1, n)

        @pl.when(end)
        def _(n=n):
            for m, part in enumerate(parts_of(1, n)):
                send_along(zsend.at[n, beyond, part], zrecv.at[n, 3, part], 1, n, 12 if m else 8 + n, near)

        if n == 0:

            @pl.when((s < 3) | (par == 1))
            def _():
                pl.semaphore_wait(round_sem.at[3], 3 - s + jnp.where(par == 1, 4, 0))

            send_edges(0)
            send_edges(1)
        if n == 1:
            pass_on(0, 0)
        if n == 2:
            pass_on(0, 1)

    def give_rest():
        for n in range(4):
            send_along(zsend.at[n, near], zrecv.at[n, 0], 2, n, n, near)

    pl.when(end)(give_rest)
    for kind, n in ((0, 2), (0, 3), (1, 0), (1, 1), (1, 2), (1, 3)):
        pass_on(kind, n)

    lane64 = iota((64, 128), 1)
    for n, (left, right) in enumerate(CHUNKS):
        drain(zrecv.at[n, pl.ds(0, 2)], zrecv_sem.at[n])
        total = zpart[n, s] + zrecv[n, 0].astype(F32) + zrecv[n, 1].astype(F32)
        zfull[:, lanes(left + 1)] = total[:, 0:128]
        zfull[:, lanes(right + 1)] = total[:, 128:256]
        for e, t in ((0, 0), (1, row - 1)):
            if t in READY[n]:

                @pl.when(par > 0 if e == 0 else par < 3)
                def _(e=e):
                    drain(hrecv.at[e], hrecv_sem.at[e])

                edge = hrecv[e, 0].astype(F32)
                for o in range(1, 4):
                    edge = edge + hrecv[e, o].astype(F32)
                for j in range(8):
                    shift = 127 - j if e == 0 else (128 - j) % 128
                    moved = edge if shift == 0 else pltpu.roll(edge, shift, 1)
                    zfull[8 * j : 8 * j + 8, lanes(0 if e == 0 else row + 1)] = moved
        for t in READY[n]:
            before, here, after = (zfull[:, lanes(t + i)] for i in range(3))
            low = jnp.where(lane64 == 0, pltpu.roll(before, 1, 1), pltpu.roll(here, 1, 1))
            high = jnp.where(lane64 == 127, pltpu.roll(after, 127, 1), pltpu.roll(here, 127, 1))
            smooth = (0.5 * here + 0.25 * (low + high)) * scale_ref[:, lanes(t)]
            for q in range(2):
                halves = [smooth[32 * h + 16 * q : 32 * h + 16 * q + 16] for h in range(2)]
                wsend[t, q] = jnp.concatenate(halves, axis=0).astype(BF16)
        if n >= 2:
            upper = n - 2
            for mine in range(2):

                @pl.when(late == mine)
                def _(upper=upper, mine=mine):
                    for i, j in STEPS:
                        if (i + j + mine + upper) % 2 == 0:
                            to_y, to_x = (y + j) % 4, (x + i) % 4
                            t = 4 * upper + 2 * (to_y % 2) + to_x // 2
                            pltpu.make_async_remote_copy(
                                wsend.at[t, to_y // 2], wrecv.at[f], send_sem.at[4], recv_sem.at[4],
                                device_id={"freq": 4 * to_y + to_x}, device_id_type=MESH,
                            ).start()
                    if mine == upper:
                        own = wsend.at[4 * upper + 2 * (y % 2) + x // 2, y // 2]
                        pltpu.make_async_copy(own, wrecv.at[f], recv_sem.at[4]).start()

    drain(wrecv, recv_sem.at[4])
    spectra = wrecv[...].reshape(512, 128)
    for half in range(2):
        rows = slice(256 * half, 256 * half + 256)
        image = jnp.dot(table_hi[rows, :], spectra, preferred_element_type=F32)
        image = image + jnp.dot(table_lo[rows, :], spectra, preferred_element_type=F32)
        isend[8 * half : 8 * half + 8] = image.astype(BF16).reshape(8, 32, 128)
        for j in (0, 1) if half == 0 else (3, 2):
            row_y = (y + 2 + j) % 4
            for i in (2, 1, 3, 0):
                if i > 0 or j != 2:
                    target_x = (x + i) % 4
                    pltpu.make_async_remote_copy(
                        isend.at[4 * j + target_x], irecv.at[slot], send_sem.at[5], recv_sem.at[5 + late],
                        device_id={"freq": 4 * row_y + target_x}, device_id_type=MESH,
                    ).start()
    pltpu.make_async_copy(isend.at[8 + x], irecv.at[slot], recv_sem.at[5 + late]).start()

    for g in range(2):
        drain(arecv.at[g, pl.ds(0, 3)], send_sem.at[g])
        drain(brecv.at[g, pl.ds(0, 7)], send_sem.at[2 + g])
    for n in range(12):
        drain(zfwd.at[0, 0], zsend_sem.at[n])

    @pl.when(par > 0)
    def _():
        drain(hsend.at[0], hsend_sem.at[0])

    @pl.when(par < 3)
    def _():
        drain(hsend.at[1], hsend_sem.at[1])

    drain(wrecv.at[pl.ds(0, 15)], send_sem.at[4])
    drain(isend.at[pl.ds(0, 15)], send_sem.at[5])
    out_copies = []
    for last in range(2):
        drain(irecv.at[pl.ds(0, 8)], recv_sem.at[5 + last])
        for q in range(2):
            for t in range(4):
                piece = irecv[8 * q + 4 * last + t, 0:26, :].astype(F32)
                out_v[last, pl.ds(2 * t + q, 26, stride=8), :] = piece
        out_copies.append(
            pltpu.make_async_copy(
                out_v.at[last, pl.ds(0, 208)].reshape(26, 8, 128), out_ref.at[:, pl.ds(8 * last, 8)], local_sem.at[last]
            )
        )
        out_copies[-1].start()
    for copy in out_copies:
        copy.wait()


def local(series, kern, prior_spectrum, prior_scale):
    sensors, params = kern.shape[2:]
    series, kern = series.transpose(2, 0, 1), kern.transpose(0, 2, 1, 3)
    vmem = pltpu.VMEM
    dma = pltpu.SemaphoreType.DMA
    operands = (series, kern, prior_spectrum, prior_scale.reshape(1, -1))
    image = pl.pallas_call(
        kernel,
        out_shape=jax.ShapeDtypeStruct((26, 16, 128), F32),
        in_specs=[
            pl.BlockSpec(memory_space=pl.ANY),
        ] * 4,
        out_specs=pl.BlockSpec(memory_space=pl.ANY),
        scratch_shapes=[
            pltpu.SMEM((16,), F32),
            vmem((1, params), F32),
            vmem((26, 8, sensors), BF16),
            vmem((2, 2, sensors, 8, params), BF16),
            vmem((2, 256, 128), F32),
            vmem((2, 32, 384), F32),
            vmem((2, 4, 32, 384), BF16),
            vmem((2, 4, 32, 384), BF16),
            vmem((2, 8, 32, 384), BF16),
            vmem((2, 2, 64, 256), BF16),
            vmem((2, 2, 64, 256 * pl.cdiv(8 * sensors, 256)), BF16),
            vmem((2, 2, 64, 256 * pl.cdiv(8 * sensors, 256)), BF16),
            vmem((4, 4, 64, 256), BF16),
            vmem((4, 4, 64, 256), F32),
            vmem((4, 2, 64, 256), BF16),
            vmem((4, 4, 64, 256), BF16),
            vmem((64, 1280), F32),
            vmem((2, 4, 8, 128), BF16),
            vmem((2, 4, 8, 128), BF16),
            vmem((8, 2, 32, 128), BF16),
            vmem((16, 32, 128), BF16),
            vmem((16, 32, 128), BF16),
            vmem((16, 32, 128), BF16),
            vmem((2, 256, 128), F32),
            vmem((512, 512), BF16),
            vmem((512, 512), BF16),
            dma((7,)),
            dma((6,)),
            dma((7,)),
            dma((12,)),
            dma((13,)),
            dma((2,)),
            dma((2,)),
            pltpu.SemaphoreType.REGULAR((4,)),
        ],
        compiler_params=pltpu.CompilerParams(
            collective_id=0, has_side_effects=True, vmem_limit_bytes=50 * 1024 * 1024
        ),
        name="adjoint",
    )(*(pltpu.with_memory_space_constraint(v, pltpu.HBM) for v in operands))
    return image.reshape(26, 8, 2, 128).transpose(0, 2, 1, 3).reshape(26, 2, params)


def solution(mesh):
    placed = (P(None, "sens", "freq"), P(None, "freq", "sens", "param"), P("freq"), P("param"))
    return jax.shard_map(
        local, mesh=mesh, in_specs=placed, out_specs=P("freq", "sens", "param"), check_vma=False
    )
```
